32 devices in a mesh: user: 16 (over z, y, x), seq: 2 (over core).
Axes of the slice: x: 2, y: 2, z: 4, core: 2. Of those that a mesh axis runs over, the one named last changes fastest.
Arguments:
- behaviors: bfloat16 [32, 2048, 256], P('user', 'seq'), may hold values from -20 to 20
- candidates: bfloat16 [32, 64, 256], P('user', 'seq'), may hold values from -64 to 64
- ranks: int32 [32, 2, 128], P('user', 'seq'), may hold values from 0 to 1151, as said below
- lengths: int32 [32], P('user'), may hold values from 1024 to 2048
- hash_planes: bfloat16 [256, 64], replicated, may hold values from -0.375 to 0.375
- norm_gain: float32 [256], replicated, may hold values from 0.5 to 1.5
- norm_bias: float32 [256], replicated, may hold values from -3 to 3
Outputs:
- interest: bfloat16 [32, 64, 256], P('user', 'seq')
The draws below stay inside these ranges and needn't reach their ends.
Inputs may be any that keep to these rules, and one draw needn't show every extreme that they name: ranks[u, s, :] are 128 distinct positions of group s's window of 1152 behaviors; on the first group all are 128 or more.
All inputs are finite; a program needn't handle non-finite values.
Results may differ from the reference program's by a relative error of at most 0.0023.
Values may be sent and summed in bfloat16 or wider, within the bound.
No kernel may reach another device: no remote copies, remote signals or barrier semaphores. Data moves between devices by JAX's collectives and lax.ppermute only.
A program may use at most 64 MiB of HBM per device.

```python
import math
import jax
import jax.numpy as jnp
from jax import lax

E = 256
BITS = 64
CANDS = 64
TOPK = 128
HALO = 128
GROUP = 1024
USERS = 32
SEQ_LEN = 2048


def user_scale(key):
    user_base = 1.0 + 2.0 * jnp.arange(USERS, dtype=jnp.float32) / (USERS - 1)
    return user_base


def raw_block(block_key, rows_count):
    array_shape = (USERS, rows_count, E)
    return jnp.clip(jax.random.normal(block_key, array_shape), -6.0, 6.0)


def first_group(key):
    return raw_block(jax.random.fold_in(key, 21), GROUP) * user_scale(key)[:, None, None]


def draw_behaviors(key, part):
    later_rows = raw_block(jax.random.fold_in(key, 22), SEQ_LEN - GROUP) * user_scale(key)[:, None, None]
    return jnp.concatenate([first_group(key), later_rows], axis=1).astype(jnp.bfloat16)


def rank_table(key):
    rank_key = jax.random.fold_in(key, 31)
    group_count = SEQ_LEN // GROUP
    row_keys = jax.random.split(rank_key, USERS * group_count)

    def pick_row(row_key, row_index):
        spread_pick = jax.random.permutation(row_key, GROUP + HALO)[:TOPK]
        first_pick = jax.random.permutation(row_key, GROUP)[:TOPK] + HALO
        return jnp.where(row_index % group_count == 0, first_pick, spread_pick)
    picks = jax.vmap(pick_row)(row_keys, jnp.arange(USERS * group_count, dtype=jnp.int32))
    return picks.reshape(USERS, group_count, TOPK).astype(jnp.int32)


def draw_ranks(key, part):
    return rank_table(key)


def draw_candidates(key, part):
    cand_key = jax.random.fold_in(key, 41)
    array_shape = (USERS, CANDS, E)
    return jnp.clip(jax.random.normal(cand_key, array_shape), -6.0, 6.0).astype(jnp.bfloat16)


def plant(entries, stream_key, smallest, high):
    longest = entries.shape.index(max(entries.shape))
    spots = []
    for shift in (0, 1):
        where = [jax.random.randint(jax.random.fold_in(stream_key, axis), (), 0, length) for axis, length in enumerate(entries.shape)]
        where[longest] = (where[longest] + shift) % entries.shape[longest]
        spots.append(tuple(where))
    return entries.at[spots[0]].set(smallest).at[spots[1]].set(high)


def centred(stream_key, shape, spread, bound, kind=jnp.bfloat16):
    return jnp.clip(spread * jax.random.normal(stream_key, shape, jnp.float32), -bound, bound).astype(kind)


def setup_inputs(seed: int = 0) -> dict:
    streams_of = jax.random.split(jax.random.key(seed), 8)
    behaviors = draw_behaviors(jax.random.fold_in(streams_of[7], 71), 0)
    candidates = draw_candidates(jax.random.fold_in(streams_of[7], 71), 0)
    ranks = draw_ranks(jax.random.fold_in(streams_of[7], 71), 0)
    lengths = plant(jax.random.randint(streams_of[3], (USERS,), GROUP, SEQ_LEN + 1), jax.random.fold_in(streams_of[3], 1), GROUP, SEQ_LEN).astype(jnp.int32)
    hash_planes = centred(streams_of[4], (E, BITS), E ** -0.5, 0.375)
    norm_gain = jnp.clip(1.0 + 0.1 * jax.random.normal(streams_of[5], (E,), jnp.float32), 0.5, 1.5)
    norm_bias = centred(streams_of[6], (E,), 0.5, 3.0, jnp.float32)
    return dict(behaviors=behaviors, candidates=candidates, ranks=ranks, lengths=lengths, hash_planes=hash_planes, norm_gain=norm_gain, norm_bias=norm_bias)


NEG_FILL = -1e+30
HASH_WEIGHT = 2.0
NORM_EPS = 1e-05

def soft_codes(rows, hash_planes):
    return jnp.tanh(jnp.dot(rows, hash_planes, preferred_element_type=jnp.float32)).astype(jnp.bfloat16)

def reference(behaviors, candidates, ranks, lengths, hash_planes, norm_gain, norm_bias):
    user_count = behaviors.shape[0]
    seq_total = behaviors.shape[1]
    feature_width = behaviors.shape[2]
    groups = ranks.shape[1]
    group_rows = seq_total // groups
    starts = jnp.arange(groups, dtype=jnp.int32) * group_rows - HALO
    position = ranks + starts[None, :, None]
    usable = (position >= 0) & (position < lengths[:, None, None])
    clipped = jnp.clip(position, 0, seq_total - 1).astype(jnp.int32).reshape(user_count, -1)
    picked = jax.vmap(lambda row_table, where_at: row_table[where_at])(behaviors, clipped)
    picked = picked.reshape(user_count, groups, -1, feature_width)
    query_codes = soft_codes(candidates, hash_planes)
    picked_codes = soft_codes(picked, hash_planes)
    code_bits = hash_planes.shape[1]
    similar = jnp.einsum('ucd,uskd->usck', candidates.astype(jnp.float32), picked.astype(jnp.float32))
    agreement = jnp.einsum('ucb,uskb->usck', query_codes.astype(jnp.float32), picked_codes.astype(jnp.float32))
    scores = similar * (1.0 / math.sqrt(feature_width)) + HASH_WEIGHT / code_bits * agreement
    usable_rows = usable[:, :, None, :]
    group_max = lax.optimization_barrier(jnp.max(jnp.where(usable_rows, scores, NEG_FILL), axis=3))
    weights = jnp.where(usable_rows, jnp.exp(scores - group_max[..., None]), 0.0)
    group_total = lax.optimization_barrier(jnp.sum(weights, axis=3))
    rounded = lax.optimization_barrier(weights.astype(jnp.bfloat16)).astype(jnp.float32)
    group_sum = jnp.einsum('usck,uskd->uscd', rounded, picked.astype(jnp.float32))
    joint_max = lax.optimization_barrier(jnp.max(group_max, axis=1))
    rescale = jnp.exp(group_max - joint_max[:, None, :])
    numerator = lax.optimization_barrier(jnp.sum(rescale[..., None] * group_sum, axis=1))
    denominator = lax.optimization_barrier(jnp.sum(rescale * group_total, axis=1))
    attended = numerator / denominator[..., None]
    row_count = user_count * candidates.shape[1]
    feature_mean = lax.optimization_barrier(jnp.sum(attended, axis=(0, 1))) / row_count
    feature_var = lax.optimization_barrier(jnp.sum(attended * attended, axis=(0, 1))) / row_count - feature_mean * feature_mean
    normed = (attended - feature_mean) * lax.rsqrt(feature_var + NORM_EPS) * norm_gain + norm_bias
    return normed.astype(jnp.bfloat16)
```

```python
import math

import jax
import jax.numpy as jnp
from jax import lax
from jax.sharding import PartitionSpec as P

HALO = 128


NEG_FILL = -1e30
HASH_WEIGHT = 2.0
NORM_EPS = 1e-05

BOTH = ("user", "seq")


def swapped_index(seq_index, seq_count):
    return seq_index ^ 1 if seq_count % 2 == 0 else seq_index


def user_total(value):
    users, seqs = lax.axis_size("user"), lax.axis_size("seq")
    if users & (users - 1):
        return lax.psum(value, "user")
    stride = 1
    while stride < users:
        pairs = [
            (user * seqs + seq, (user ^ stride) * seqs + swapped_index(seq, seqs))
            for user in range(users)
            for seq in range(seqs)
        ]
        value = value + lax.ppermute(value, BOTH, pairs)
        stride *= 2
    return value


def seq_parts(value):
    seqs = lax.axis_size("seq")
    if seqs == 2:
        return [value, lax.ppermute(value, "seq", [(0, 1), (1, 0)])]
    everything = lax.all_gather(value, "seq")
    return [everything[k] for k in range(seqs)]


def soft_codes(rows, hash_planes):
    return jnp.tanh(jnp.dot(rows, hash_planes, preferred_element_type=jnp.float32)).astype(
        jnp.bfloat16
    )


def shards(behaviors, candidates, ranks, lengths, hash_planes, norm_gain, norm_bias):
    group_rows = behaviors.shape[1]
    feature_width = behaviors.shape[2]
    own_cands = candidates.shape[1]
    code_bits = hash_planes.shape[1]
    seqs = lax.axis_size("seq")
    seq_index = lax.axis_index("seq")
    tail_rows = behaviors[:, group_rows - HALO :, :]
    before = lax.ppermute(tail_rows, "seq", [(k, (k + 1) % seqs) for k in range(seqs)])
    queries = lax.all_gather(candidates, "seq", axis=1, tiled=True)
    window_pos = ranks[:, 0, :]
    from_tail = window_pos < HALO
    tail_index = jnp.clip(window_pos, 0, HALO - 1)
    own_index = jnp.clip(window_pos - HALO, 0, group_rows - 1)
    take_rows = jax.vmap(lambda row_table, where_at: row_table[where_at])
    picked = jnp.where(
        from_tail[:, :, None], take_rows(before, tail_index), take_rows(behaviors, own_index)
    )
    position = seq_index * group_rows - HALO + window_pos
    usable = (position >= 0) & (position < lengths[:, None])
    query_codes = soft_codes(queries, hash_planes)
    picked_codes = soft_codes(picked, hash_planes)
    similar = jnp.einsum("ucd,ukd->uck", queries, picked, preferred_element_type=jnp.float32)
    agreement = jnp.einsum(
        "ucb,ukb->uck", query_codes, picked_codes, preferred_element_type=jnp.float32
    )
    scores = similar * (1.0 / math.sqrt(feature_width)) + HASH_WEIGHT / code_bits * agreement
    usable_rows = usable[:, None, :]
    group_max = jnp.max(jnp.where(usable_rows, scores, NEG_FILL), axis=2)
    weights = jnp.where(usable_rows, jnp.exp(scores - group_max[..., None]), 0.0)
    group_total = jnp.sum(weights, axis=2)
    group_sum = jnp.einsum(
        "uck,ukd->ucd", weights.astype(jnp.bfloat16), picked, preferred_element_type=jnp.float32
    )
    cands = group_sum.shape[1]
    side = jnp.broadcast_to(
        jnp.stack([group_max, group_total], axis=2)[..., None], group_sum.shape[:2] + (2, 64)
    ).reshape(group_sum.shape[:2] + (128,))
    parts = seq_parts(jnp.concatenate([group_sum, side], axis=2))
    tops = [part[:, :, feature_width] for part in parts]
    joint_max = tops[0]
    for top in tops[1:]:
        joint_max = jnp.maximum(joint_max, top)
    numerator, denominator = 0.0, 0.0
    for part, top in zip(parts, tops):
        rescale = jnp.exp(top - joint_max)
        numerator = numerator + rescale[..., None] * part[:, :, :feature_width]
        denominator = denominator + rescale * part[:, :, feature_width + 64]
    attended = numerator / denominator[..., None]
    moments = user_total(
        jnp.stack([jnp.sum(attended, axis=(0, 1)), jnp.sum(attended * attended, axis=(0, 1))])
    )
    row_count = attended.shape[0] * cands * lax.axis_size("user")
    feature_mean = moments[0] / row_count
    feature_var = moments[1] / row_count - feature_mean * feature_mean
    own = lax.dynamic_slice_in_dim(attended, seq_index * own_cands, own_cands, 1)
    normed = (own - feature_mean) * lax.rsqrt(feature_var + NORM_EPS) * norm_gain + norm_bias
    return normed.astype(jnp.bfloat16)


def solution(mesh):
    in_specs = (
        P("user", "seq", None),
        P("user", "seq", None),
        P("user", "seq", None),
        P("user"),
        P(),
        P(),
        P(),
    )
    out_specs = P("user", "seq", None)
    return jax.shard_map(shards, mesh=mesh, in_specs=in_specs, out_specs=out_specs, check_vma=False)
```

```python
import math

import jax
import jax.numpy as jnp
from jax import lax
from jax.experimental import pallas as pl
from jax.experimental.pallas import tpu as pltpu
from jax.sharding import PartitionSpec as P

HALO = 128


NEG_FILL = -1e30
HASH_WEIGHT = 2.0
NORM_EPS = 1e-05

BOTH = ("user", "seq")
SIDE = 128
CHUNK = 256
VMEM_LIMIT = 8 * 1024 * 1024


def user_total(value):
    users, seqs = lax.axis_size("user"), lax.axis_size("seq")
    if users & (users - 1):
        return lax.psum(value, "user")
    stride = 1
    while stride < users:
        pairs = [
            (user * seqs + seq, (user ^ stride) * seqs + (seq ^ 1 if seqs % 2 == 0 else seq))
            for user in range(users)
            for seq in range(seqs)
        ]
        value = value + lax.ppermute(value, BOTH, pairs)
        stride *= 2
    return value


def last_with_last(left, right):
    return lax.dot_general(
        left, right, (((1,), (1,)), ((), ())), preferred_element_type=jnp.float32
    )


def soft_codes(rows, hash_planes):
    return jnp.tanh(jnp.dot(rows, hash_planes, preferred_element_type=jnp.float32)).astype(
        jnp.bfloat16
    )


def normalized(own, moments, row_count, norm_gain, norm_bias):
    feature_mean = moments[0] / row_count
    feature_var = moments[1] / row_count - feature_mean * feature_mean
    normed = (own - feature_mean) * lax.rsqrt(feature_var + NORM_EPS) * norm_gain + norm_bias
    return normed.astype(jnp.bfloat16)


def any_groups(behaviors, candidates, ranks, lengths, hash_planes, norm_gain, norm_bias):
    group_rows = behaviors.shape[1]
    feature_width = behaviors.shape[2]
    own_cands = candidates.shape[1]
    code_bits = hash_planes.shape[1]
    seqs = lax.axis_size("seq")
    seq_index = lax.axis_index("seq")
    tail_rows = behaviors[:, group_rows - HALO :, :]
    before = lax.ppermute(tail_rows, "seq", [(k, (k + 1) % seqs) for k in range(seqs)])
    queries = lax.all_gather(candidates, "seq", axis=1, tiled=True)
    window_pos = ranks[:, 0, :]
    from_tail = window_pos < HALO
    tail_index = jnp.clip(window_pos, 0, HALO - 1)
    own_index = jnp.clip(window_pos - HALO, 0, group_rows - 1)
    take_rows = jax.vmap(lambda row_table, where_at: row_table[where_at])
    picked = jnp.where(
        from_tail[:, :, None], take_rows(before, tail_index), take_rows(behaviors, own_index)
    )
    position = seq_index * group_rows - HALO + window_pos
    usable = (position >= 0) & (position < lengths[:, None])
    query_codes = soft_codes(queries, hash_planes)
    picked_codes = soft_codes(picked, hash_planes)
    similar = jnp.einsum("ucd,ukd->uck", queries, picked, preferred_element_type=jnp.float32)
    agreement = jnp.einsum(
        "ucb,ukb->uck", query_codes, picked_codes, preferred_element_type=jnp.float32
    )
    scores = similar * (1.0 / math.sqrt(feature_width)) + HASH_WEIGHT / code_bits * agreement
    usable_rows = usable[:, None, :]
    group_max = jnp.max(jnp.where(usable_rows, scores, NEG_FILL), axis=2)
    weights = jnp.where(usable_rows, jnp.exp(scores - group_max[..., None]), 0.0)
    group_total = jnp.sum(weights, axis=2)
    group_sum = jnp.einsum(
        "uck,ukd->ucd", weights.astype(jnp.bfloat16), picked, preferred_element_type=jnp.float32
    )
    tops = lax.all_gather(group_max, "seq")
    rescales = jnp.exp(tops - jnp.max(tops, axis=0))
    numerator = jnp.sum(rescales[..., None] * lax.all_gather(group_sum, "seq"), axis=0)
    denominator = jnp.sum(rescales * lax.all_gather(group_total, "seq"), axis=0)
    attended = numerator / denominator[..., None]
    moments = user_total(
        jnp.stack([jnp.sum(attended, axis=(0, 1)), jnp.sum(attended * attended, axis=(0, 1))])
    )
    row_count = attended.shape[0] * attended.shape[1] * lax.axis_size("user")
    own = lax.dynamic_slice_in_dim(attended, seq_index * own_cands, own_cands, 1)
    return normalized(own, moments, row_count, norm_gain, norm_bias)


def rank_columns(rank_row, picks):
    return jnp.transpose(jnp.broadcast_to(rank_row, (picks, picks)))


def own_picks_kernel(
    ranks_ref, lengths_ref, norm_gain_ref, norm_bias_ref, behaviors_hbm,
    picked_ref, live_ref, gain_ref, bias_ref,
    rows, row_sem,
):
    users, group_rows, _ = behaviors_hbm.shape
    picks = ranks_ref.shape[2]
    chunks = group_rows // CHUNK
    loads = []
    for user in range(users):
        for chunk in range(chunks):
            part = (user, pl.ds(chunk * CHUNK, CHUNK))
            loads.append(
                pltpu.make_async_copy(
                    behaviors_hbm.at[part], rows.at[part], row_sem.at[user * chunks + chunk]
                )
            )
            loads[-1].start()
    start = lax.axis_index("seq") * group_rows - HALO
    gain_ref[...] = norm_gain_ref[...]
    bias_ref[...] = norm_bias_ref[...]
    lanes = lax.broadcasted_iota(jnp.int32, (picks, CHUNK), 1)
    for user in range(users):
        position = ranks_ref[user] + start
        usable = (position >= 0) & (position < lengths_ref[user])
        live_ref[user] = usable.astype(jnp.float32)
        columns = rank_columns(ranks_ref[user], picks)
        wide = jnp.concatenate([columns] * (CHUNK // picks), axis=1) - HALO
        found = jnp.zeros((picks, rows.shape[2]), jnp.float32)
        for chunk in range(chunks):
            loads[user * chunks + chunk].wait()
            chosen = (wide == lanes + chunk * CHUNK).astype(jnp.float32).astype(jnp.bfloat16)
            found += jnp.dot(
                chosen,
                rows[user, chunk * CHUNK : (chunk + 1) * CHUNK],
                preferred_element_type=jnp.float32,
            )
        picked_ref[user] = found.astype(jnp.bfloat16)


def attend_kernel(ranks_ref, live_ref, picked_ref, mine_ref, other_ref, planes_ref, part_ref):
    users, picks, feature_width = picked_ref.shape
    code_bits = planes_ref.shape[0]
    planes = planes_ref[...]
    lanes = lax.broadcasted_iota(jnp.int32, (picks, HALO), 1)
    for user in range(users):
        chosen = rank_columns(ranks_ref[user], picks) == lanes
        from_tail = jnp.dot(
            chosen.astype(jnp.float32).astype(jnp.bfloat16),
            other_ref[user, :HALO],
            preferred_element_type=jnp.float32,
        )
        picked = (picked_ref[user].astype(jnp.float32) + from_tail).astype(jnp.bfloat16)
        queries = jnp.concatenate([mine_ref[user], other_ref[user, HALO:]], axis=0)
        query_codes = jnp.tanh(last_with_last(queries, planes)).astype(jnp.bfloat16)
        picked_codes = jnp.tanh(last_with_last(picked, planes)).astype(jnp.bfloat16)
        similar = last_with_last(queries, picked)
        agreement = last_with_last(query_codes, picked_codes)
        scores = similar * (1.0 / math.sqrt(feature_width)) + HASH_WEIGHT / code_bits * agreement
        usable = live_ref[user] > 0.0
        group_max = jnp.max(jnp.where(usable, scores, NEG_FILL), axis=1, keepdims=True)
        weights = jnp.where(usable, jnp.exp(scores - group_max), 0.0)
        group_total = jnp.sum(weights, axis=1, keepdims=True)
        part_ref[user, :, :feature_width] = jnp.dot(
            weights.astype(jnp.bfloat16), picked, preferred_element_type=jnp.float32
        )
        side_lane = lax.broadcasted_iota(jnp.int32, (queries.shape[0], SIDE), 1)
        part_ref[user, :, feature_width:] = jnp.where(
            side_lane < SIDE // 2, group_max, group_total
        )


def merge_kernel(mine_ref, other_ref, own_ref, moments_ref):
    users, cands, packed = mine_ref.shape
    width = packed - SIDE
    half = cands // 2
    sums = jnp.zeros((1, width), jnp.float32)
    squares = jnp.zeros((1, width), jnp.float32)
    for user in range(users):
        for first in (0, half):
            left = mine_ref[user, first : first + half]
            right = other_ref[user, half - first : cands - first]
            left_top, right_top = left[:, width : width + 1], right[:, width : width + 1]
            last = width + SIDE // 2
            joint_max = jnp.maximum(left_top, right_top)
            left_scale = jnp.exp(left_top - joint_max)
            right_scale = jnp.exp(right_top - joint_max)
            numerator = left_scale * left[:, :width] + right_scale * right[:, :width]
            denominator = (
                left_scale * left[:, last : last + 1] + right_scale * right[:, last : last + 1]
            )
            attended = numerator / denominator
            sums += jnp.sum(attended, axis=0, keepdims=True)
            squares += jnp.sum(attended * attended, axis=0, keepdims=True)
            if first == 0:
                own_ref[user] = attended
    moments_ref[0:1] = sums
    moments_ref[1:2] = squares


def two_groups(behaviors, candidates, ranks, lengths, hash_planes, norm_gain, norm_bias):
    users, group_rows, width = behaviors.shape
    own_cands = candidates.shape[1]
    picks = ranks.shape[2]
    cands = 2 * own_cands
    f32, bf16 = jnp.float32, jnp.bfloat16
    in_vmem = pl.BlockSpec(memory_space=pltpu.VMEM)
    swap = [(0, 1), (1, 0)]
    other = lax.ppermute(
        jnp.concatenate([behaviors[:, group_rows - HALO :], candidates], axis=1), "seq", swap
    )
    loads = users * group_rows // CHUNK
    picked, live, gain, bias = pl.pallas_call(
        own_picks_kernel,
        out_shape=(
            jax.ShapeDtypeStruct((users, picks, width), bf16),
            jax.ShapeDtypeStruct((users, 1, picks), f32),
            jax.ShapeDtypeStruct(norm_gain.shape, f32),
            jax.ShapeDtypeStruct(norm_bias.shape, f32),
        ),
        in_specs=[
            in_vmem,
            pl.BlockSpec(memory_space=pltpu.SMEM),
            in_vmem,
            in_vmem,
            pl.BlockSpec(memory_space=pl.ANY),
        ],
        out_specs=(in_vmem,) * 4,
        scratch_shapes=[
            pltpu.VMEM(behaviors.shape, bf16),
            pltpu.SemaphoreType.DMA((loads,)),
        ],
        cost_estimate=pl.CostEstimate(
            flops=2 * users * picks * group_rows * width,
            bytes_accessed=behaviors.nbytes,
            transcendentals=0,
        ),
        compiler_params=pltpu.CompilerParams(vmem_limit_bytes=VMEM_LIMIT),
        name="own_picks",
    )(
        ranks,
        lengths,
        norm_gain,
        norm_bias,
        pltpu.with_memory_space_constraint(behaviors, pltpu.HBM),
    )
    part = pl.pallas_call(
        attend_kernel,
        out_shape=jax.ShapeDtypeStruct((users, cands, width + SIDE), f32),
        in_specs=[in_vmem] * 6,
        out_specs=in_vmem,
        compiler_params=pltpu.CompilerParams(vmem_limit_bytes=VMEM_LIMIT),
        name="attend",
    )(ranks, live, picked, candidates, other, hash_planes.T)
    own, moments = pl.pallas_call(
        merge_kernel,
        out_shape=(
            jax.ShapeDtypeStruct((users, own_cands, width), f32),
            jax.ShapeDtypeStruct((2, width), f32),
        ),
        in_specs=[in_vmem] * 2,
        out_specs=(in_vmem,) * 2,
        compiler_params=pltpu.CompilerParams(vmem_limit_bytes=VMEM_LIMIT),
        name="merge",
    )(part, lax.ppermute(part, "seq", swap))
    row_count = users * cands * lax.axis_size("user")
    return normalized(own, user_total(moments), row_count, gain, bias)


def solution(mesh):
    in_specs = (
        P("user", "seq", None),
        P("user", "seq", None),
        P("user", "seq", None),
        P("user"),
        P(),
        P(),
        P(),
    )
    out_specs = P("user", "seq", None)
    shards = two_groups if mesh.shape["seq"] == 2 else any_groups
    return jax.shard_map(shards, mesh=mesh, in_specs=in_specs, out_specs=out_specs, check_vma=False)
```

```python
import math

import jax
import jax.numpy as jnp
from jax import lax
from jax.experimental import pallas as pl
from jax.experimental.pallas import tpu as pltpu
from jax.sharding import PartitionSpec as P

HALO = 128


NEG_FILL = -1e30
HASH_WEIGHT = 2.0
NORM_EPS = 1e-05

BOTH = ("user", "seq")
SIDE = 128
CHUNK = 1024
TAIL_CHUNK = 128
VMEM_LIMIT = 8 * 1024 * 1024


def user_total(value):
    users, seqs = lax.axis_size("user"), lax.axis_size("seq")
    if users & (users - 1):
        return lax.psum(value, "user")
    stride = 1
    while stride < users:
        pairs = [
            (user * seqs + seq, (user ^ stride) * seqs + (seq ^ 1 if seqs % 2 == 0 else seq))
            for user in range(users)
            for seq in range(seqs)
        ]
        value = value + lax.ppermute(value, BOTH, pairs)
        stride *= 2
    return value


def last_with_last(left, right):
    return lax.dot_general(
        left, right, (((1,), (1,)), ((), ())), preferred_element_type=jnp.float32
    )


def soft_codes(rows, planes):
    return jnp.tanh(last_with_last(rows, planes)).astype(jnp.bfloat16)


def normalized(own, moments, row_count, norm_gain, norm_bias):
    feature_mean = moments[0] / row_count
    feature_var = moments[1] / row_count - feature_mean * feature_mean
    normed = (own - feature_mean) * lax.rsqrt(feature_var + NORM_EPS) * norm_gain + norm_bias
    return normed.astype(jnp.bfloat16)


def any_groups(behaviors, candidates, ranks, lengths, hash_planes, norm_gain, norm_bias):
    group_rows = behaviors.shape[1]
    feature_width = behaviors.shape[2]
    own_cands = candidates.shape[1]
    code_bits = hash_planes.shape[1]
    seqs = lax.axis_size("seq")
    seq_index = lax.axis_index("seq")
    tail_rows = behaviors[:, group_rows - HALO :, :]
    before = lax.ppermute(tail_rows, "seq", [(k, (k + 1) % seqs) for k in range(seqs)])
    queries = lax.all_gather(candidates, "seq", axis=1, tiled=True)
    window_pos = ranks[:, 0, :]
    from_tail = window_pos < HALO
    tail_index = jnp.clip(window_pos, 0, HALO - 1)
    own_index = jnp.clip(window_pos - HALO, 0, group_rows - 1)
    take_rows = jax.vmap(lambda row_table, where_at: row_table[where_at])
    picked = jnp.where(
        from_tail[:, :, None], take_rows(before, tail_index), take_rows(behaviors, own_index)
    )
    position = seq_index * group_rows - HALO + window_pos
    usable = (position >= 0) & (position < lengths[:, None])
    query_codes, picked_codes = (
        jnp.tanh(
            jnp.einsum("ukd,db->ukb", rows, hash_planes, preferred_element_type=jnp.float32)
        ).astype(jnp.bfloat16)
        for rows in (queries, picked)
    )
    similar = jnp.einsum("ucd,ukd->uck", queries, picked, preferred_element_type=jnp.float32)
    agreement = jnp.einsum(
        "ucb,ukb->uck", query_codes, picked_codes, preferred_element_type=jnp.float32
    )
    scores = similar * (1.0 / math.sqrt(feature_width)) + HASH_WEIGHT / code_bits * agreement
    usable_rows = usable[:, None, :]
    group_max = jnp.max(jnp.where(usable_rows, scores, NEG_FILL), axis=2)
    weights = jnp.where(usable_rows, jnp.exp(scores - group_max[..., None]), 0.0)
    group_total = jnp.sum(weights, axis=2)
    group_sum = jnp.einsum(
        "uck,ukd->ucd", weights.astype(jnp.bfloat16), picked, preferred_element_type=jnp.float32
    )
    tops = lax.all_gather(group_max, "seq")
    rescales = jnp.exp(tops - jnp.max(tops, axis=0))
    numerator = jnp.sum(rescales[..., None] * lax.all_gather(group_sum, "seq"), axis=0)
    denominator = jnp.sum(rescales * lax.all_gather(group_total, "seq"), axis=0)
    attended = numerator / denominator[..., None]
    moments = user_total(
        jnp.stack([jnp.sum(attended, axis=(0, 1)), jnp.sum(attended * attended, axis=(0, 1))])
    )
    row_count = attended.shape[0] * attended.shape[1] * lax.axis_size("user")
    own = lax.dynamic_slice_in_dim(attended, seq_index * own_cands, own_cands, 1)
    return normalized(own, moments, row_count, norm_gain, norm_bias)


def load_kernel(
    ranks_hbm, lengths_hbm, norm_gain_hbm, norm_bias_hbm, planes_hbm, mine_hbm, behaviors_hbm,
    sent_ref, rows_ref, mine_ref, places_ref, gain_ref, bias_ref, planes_ref,
    ranks, lengths, sems,
):
    users, group_rows, _ = behaviors_hbm.shape
    tail = group_rows - HALO
    pairs = [
        (ranks_hbm, ranks),
        (lengths_hbm, lengths),
        (planes_hbm, planes_ref),
        (mine_hbm, mine_ref),
        (mine_hbm, sent_ref.at[:, pl.ds(HALO, mine_ref.shape[1])]),
        (norm_gain_hbm, gain_ref),
        (norm_bias_hbm, bias_ref),
    ]
    for user in range(users):
        for first in range(0, HALO, TAIL_CHUNK):
            pairs.append(
                (
                    behaviors_hbm.at[user, pl.ds(tail + first, TAIL_CHUNK)],
                    sent_ref.at[user, pl.ds(first, TAIL_CHUNK)],
                )
            )
    for user in range(users):
        for first in range(0, group_rows, CHUNK):
            part = (user, pl.ds(first, CHUNK))
            pairs.append((behaviors_hbm.at[part], rows_ref.at[part]))
    copies = [
        pltpu.make_async_copy(source, target, sems.at[k])
        for k, (source, target) in enumerate(pairs)
    ]
    for copy in copies:
        copy.start()
    for copy in copies[:2]:
        copy.wait()
    start = lax.axis_index("seq") * group_rows - HALO
    for user in range(users):
        position = ranks[user] + start
        usable = (position >= 0) & (position < lengths[user])
        places_ref[user] = jnp.where(usable, ranks[user], HALO + group_rows)
    for copy in copies[2:]:
        copy.wait()


def own_picks_kernel(
    places_ref, rows_ref, mine_ref, planes_ref,
    picked_ref, picked_codes_ref, mine_codes_ref, masks_ref,
):
    users, group_rows, _ = rows_ref.shape
    picks = places_ref.shape[2]
    planes = planes_ref[...]
    lanes = lax.broadcasted_iota(jnp.int32, (picks, group_rows), 1)
    for user in range(users):
        places = places_ref[user]
        columns = jnp.transpose(jnp.broadcast_to(places, (picks, picks)))
        in_tail = (columns == lanes[:, :HALO]).astype(jnp.float32)
        masks_ref[user, 0:1] = ((places >= HALO) & (places < HALO + group_rows)).astype(jnp.float32)
        masks_ref[user, 1:2] = jnp.max(in_tail, axis=0, keepdims=True)
        wide = jnp.concatenate([columns - HALO] * (group_rows // picks), axis=1)
        chosen = (wide == lanes).astype(jnp.float32).astype(jnp.bfloat16)
        picked = jnp.dot(chosen, rows_ref[user], preferred_element_type=jnp.float32).astype(
            jnp.bfloat16
        )
        picked_ref[user] = picked
        picked_codes_ref[user] = soft_codes(picked, planes)
        mine_codes_ref[user] = soft_codes(mine_ref[user], planes)


def attend_kernel(
    masks_ref, picked_ref, picked_codes_ref, mine_ref, mine_codes_ref, other_ref, planes_ref,
    part_ref,
):
    users, _, width = picked_ref.shape
    code_bits = planes_ref.shape[0]
    planes = planes_ref[...]
    for user in range(users):
        codes = soft_codes(other_ref[user], planes)
        queries = jnp.concatenate([mine_ref[user], other_ref[user, HALO:]], axis=0)
        query_codes = jnp.concatenate([mine_codes_ref[user], codes[HALO:]], axis=0)
        rows = jnp.concatenate([picked_ref[user], other_ref[user, :HALO]], axis=0)
        row_codes = jnp.concatenate([picked_codes_ref[user], codes[:HALO]], axis=0)
        similar = last_with_last(queries, rows)
        agreement = last_with_last(query_codes, row_codes)
        scores = similar * (1.0 / math.sqrt(width)) + HASH_WEIGHT / code_bits * agreement
        usable = jnp.concatenate([masks_ref[user, 0:1], masks_ref[user, 1:2]], axis=1) > 0.0
        group_max = jnp.max(jnp.where(usable, scores, NEG_FILL), axis=1, keepdims=True)
        weights = jnp.where(usable, jnp.exp(scores - group_max), 0.0)
        group_total = jnp.sum(weights, axis=1, keepdims=True)
        part_ref[user, :, :width] = jnp.dot(
            weights.astype(jnp.bfloat16), rows, preferred_element_type=jnp.float32
        )
        side_lane = lax.broadcasted_iota(jnp.int32, (queries.shape[0], SIDE), 1)
        part_ref[user, :, width:] = jnp.where(side_lane < SIDE // 2, group_max, group_total)


def merge_kernel(mine_ref, other_ref, own_ref, moments_ref):
    users, cands, packed = mine_ref.shape
    width = packed - SIDE
    half = cands // 2
    sums = jnp.zeros((1, width), jnp.float32)
    squares = jnp.zeros((1, width), jnp.float32)
    for user in range(users):
        for first in (0, half):
            left = mine_ref[user, first : first + half]
            right = other_ref[user, half - first : cands - first]
            left_top, right_top = left[:, width : width + 1], right[:, width : width + 1]
            last = width + SIDE // 2
            joint_max = jnp.maximum(left_top, right_top)
            left_scale = jnp.exp(left_top - joint_max)
            right_scale = jnp.exp(right_top - joint_max)
            numerator = left_scale * left[:, :width] + right_scale * right[:, :width]
            denominator = (
                left_scale * left[:, last : last + 1] + right_scale * right[:, last : last + 1]
            )
            attended = numerator / denominator
            sums += jnp.sum(attended, axis=0, keepdims=True)
            squares += jnp.sum(attended * attended, axis=0, keepdims=True)
            if first == 0:
                own_ref[user] = attended
    moments_ref[0:1] = sums
    moments_ref[1:2] = squares


def two_groups(behaviors, candidates, ranks, lengths, hash_planes, norm_gain, norm_bias):
    users, group_rows, width = behaviors.shape
    own_cands = candidates.shape[1]
    picks = ranks.shape[2]
    cands = 2 * own_cands
    f32, bf16 = jnp.float32, jnp.bfloat16
    in_vmem = pl.BlockSpec(memory_space=pltpu.VMEM)
    swap = [(0, 1), (1, 0)]
    bits = hash_planes.shape[1]
    arguments = (ranks, lengths, norm_gain, norm_bias, hash_planes.T, candidates, behaviors)
    params = pltpu.CompilerParams(vmem_limit_bytes=VMEM_LIMIT)
    sent, rows, mine, places, gain, bias, planes = pl.pallas_call(
        load_kernel,
        out_shape=(
            jax.ShapeDtypeStruct((users, HALO + own_cands, width), bf16),
            jax.ShapeDtypeStruct(behaviors.shape, bf16),
            jax.ShapeDtypeStruct(candidates.shape, bf16),
            jax.ShapeDtypeStruct(ranks.shape, jnp.int32),
            jax.ShapeDtypeStruct(norm_gain.shape, f32),
            jax.ShapeDtypeStruct(norm_bias.shape, f32),
            jax.ShapeDtypeStruct((bits, width), bf16),
        ),
        in_specs=[pl.BlockSpec(memory_space=pl.ANY)] * len(arguments),
        out_specs=(in_vmem,) * 7,
        scratch_shapes=[
            pltpu.VMEM(ranks.shape, jnp.int32),
            pltpu.SMEM(lengths.shape, jnp.int32),
            pltpu.SemaphoreType.DMA((7 + users * (HALO // TAIL_CHUNK + group_rows // CHUNK),)),
        ],
        compiler_params=params,
        name="load",
    )(*(pltpu.with_memory_space_constraint(value, pltpu.HBM) for value in arguments))
    other = lax.ppermute(sent, "seq", swap)
    picked, picked_codes, mine_codes, masks = pl.pallas_call(
        own_picks_kernel,
        out_shape=(
            jax.ShapeDtypeStruct((users, picks, width), bf16),
            jax.ShapeDtypeStruct((users, picks, bits), bf16),
            jax.ShapeDtypeStruct((users, own_cands, bits), bf16),
            jax.ShapeDtypeStruct((users, 2, picks), f32),
        ),
        in_specs=[in_vmem] * 4,
        out_specs=(in_vmem,) * 4,
        cost_estimate=pl.CostEstimate(
            flops=2 * users * picks * group_rows * width,
            bytes_accessed=behaviors.nbytes,
            transcendentals=0,
        ),
        compiler_params=params,
        name="own_picks",
    )(places, rows, mine, planes)
    part = pl.pallas_call(
        attend_kernel,
        out_shape=jax.ShapeDtypeStruct((users, cands, width + SIDE), f32),
        in_specs=[in_vmem] * 7,
        out_specs=in_vmem,
        compiler_params=params,
        name="attend",
    )(masks, picked, picked_codes, mine, mine_codes, other, planes)
    own, moments = pl.pallas_call(
        merge_kernel,
        out_shape=(
            jax.ShapeDtypeStruct((users, own_cands, width), f32),
            jax.ShapeDtypeStruct((2, width), f32),
        ),
        in_specs=[in_vmem] * 2,
        out_specs=(in_vmem,) * 2,
        compiler_params=params,
        name="merge",
    )(part, lax.ppermute(part, "seq", swap))
    row_count = users * cands * lax.axis_size("user")
    return normalized(own, user_total(moments), row_count, gain, bias)


def solution(mesh):
    in_specs = (
        P("user", "seq", None),
        P("user", "seq", None),
        P("user", "seq", None),
        P("user"),
        P(),
        P(),
        P(),
    )
    out_specs = P("user", "seq", None)
    shards = two_groups if mesh.shape["seq"] == 2 else any_groups
    return jax.shard_map(shards, mesh=mesh, in_specs=in_specs, out_specs=out_specs, check_vma=False)
```

```python
import math

import jax
import jax.numpy as jnp
from jax import lax
from jax.experimental import pallas as pl
from jax.experimental.pallas import tpu as pltpu
from jax.sharding import PartitionSpec as P

HALO = 128


NEG_FILL = -1e30
HASH_WEIGHT = 2.0
NORM_EPS = 1e-05

BOTH = ("user", "seq")
SIDE = 128
VMEM_LIMIT = 8 * 1024 * 1024
LOAD_COST = 10**8


def user_total(value):
    users, seqs = lax.axis_size("user"), lax.axis_size("seq")
    if users & (users - 1):
        return lax.psum(value, "user")
    stride = 1
    while stride < users:
        pairs = [
            (user * seqs + seq, (user ^ stride) * seqs + (seq ^ 1 if seqs % 2 == 0 else seq))
            for user in range(users)
            for seq in range(seqs)
        ]
        value = value + lax.ppermute(value, BOTH, pairs)
        stride *= 2
    return value


def last_with_last(left, right):
    return lax.dot_general(
        left, right, (((1,), (1,)), ((), ())), preferred_element_type=jnp.float32
    )


def soft_codes(rows, planes):
    return jnp.tanh(last_with_last(rows, planes)).astype(jnp.bfloat16)


def normalized(own, moments, row_count, norm_gain, norm_bias):
    feature_mean = moments[0] / row_count
    feature_var = moments[1] / row_count - feature_mean * feature_mean
    normed = (own - feature_mean) * lax.rsqrt(feature_var + NORM_EPS) * norm_gain + norm_bias
    return normed.astype(jnp.bfloat16)


def any_groups(behaviors, candidates, ranks, lengths, hash_planes, norm_gain, norm_bias):
    group_rows = behaviors.shape[1]
    feature_width = behaviors.shape[2]
    own_cands = candidates.shape[1]
    code_bits = hash_planes.shape[1]
    seqs = lax.axis_size("seq")
    seq_index = lax.axis_index("seq")
    tail_rows = behaviors[:, group_rows - HALO :, :]
    before = lax.ppermute(tail_rows, "seq", [(k, (k + 1) % seqs) for k in range(seqs)])
    queries = lax.all_gather(candidates, "seq", axis=1, tiled=True)
    window_pos = ranks[:, 0, :]
    from_tail = window_pos < HALO
    tail_index = jnp.clip(window_pos, 0, HALO - 1)
    own_index = jnp.clip(window_pos - HALO, 0, group_rows - 1)
    take_rows = jax.vmap(lambda row_table, where_at: row_table[where_at])
    picked = jnp.where(
        from_tail[:, :, None], take_rows(before, tail_index), take_rows(behaviors, own_index)
    )
    position = seq_index * group_rows - HALO + window_pos
    usable = (position >= 0) & (position < lengths[:, None])
    query_codes, picked_codes = (
        jnp.tanh(
            jnp.einsum("ukd,db->ukb", rows, hash_planes, preferred_element_type=jnp.float32)
        ).astype(jnp.bfloat16)
        for rows in (queries, picked)
    )
    similar = jnp.einsum("ucd,ukd->uck", queries, picked, preferred_element_type=jnp.float32)
    agreement = jnp.einsum(
        "ucb,ukb->uck", query_codes, picked_codes, preferred_element_type=jnp.float32
    )
    scores = similar * (1.0 / math.sqrt(feature_width)) + HASH_WEIGHT / code_bits * agreement
    usable_rows = usable[:, None, :]
    group_max = jnp.max(jnp.where(usable_rows, scores, NEG_FILL), axis=2)
    weights = jnp.where(usable_rows, jnp.exp(scores - group_max[..., None]), 0.0)
    group_total = jnp.sum(weights, axis=2)
    group_sum = jnp.einsum(
        "uck,ukd->ucd", weights.astype(jnp.bfloat16), picked, preferred_element_type=jnp.float32
    )
    tops = lax.all_gather(group_max, "seq")
    rescales = jnp.exp(tops - jnp.max(tops, axis=0))
    numerator = jnp.sum(rescales[..., None] * lax.all_gather(group_sum, "seq"), axis=0)
    denominator = jnp.sum(rescales * lax.all_gather(group_total, "seq"), axis=0)
    attended = numerator / denominator[..., None]
    moments = user_total(
        jnp.stack([jnp.sum(attended, axis=(0, 1)), jnp.sum(attended * attended, axis=(0, 1))])
    )
    row_count = attended.shape[0] * attended.shape[1] * lax.axis_size("user")
    own = lax.dynamic_slice_in_dim(attended, seq_index * own_cands, own_cands, 1)
    return normalized(own, moments, row_count, norm_gain, norm_bias)


def load_kernel(
    ranks_hbm, lengths_hbm, norm_gain_hbm, norm_bias_hbm, planes_hbm, mine_hbm, behaviors_hbm,
    sent_ref, places_ref, gain_ref, bias_ref, planes_ref,
    ranks, lengths, sems,
):
    users, group_rows, _ = behaviors_hbm.shape
    tail = group_rows - HALO
    pairs = [
        (ranks_hbm, ranks),
        (lengths_hbm, lengths),
        (mine_hbm, sent_ref.at[:, pl.ds(HALO, mine_hbm.shape[1])]),
        (behaviors_hbm.at[:, pl.ds(tail, HALO)], sent_ref.at[:, pl.ds(0, HALO)]),
        (planes_hbm, planes_ref),
        (norm_gain_hbm, gain_ref),
        (norm_bias_hbm, bias_ref),
    ]
    copies = [
        pltpu.make_async_copy(source, target, sems.at[k])
        for k, (source, target) in enumerate(pairs)
    ]
    for copy in copies:
        copy.start()
    for copy in copies[:2]:
        copy.wait()
    start = lax.axis_index("seq") * group_rows - HALO
    for user in range(users):
        position = ranks[user] + start
        usable = (position >= 0) & (position < lengths[user])
        places_ref[user] = jnp.where(usable, ranks[user], HALO + group_rows)
    for copy in copies[2:]:
        copy.wait()


def own_picks_kernel(
    places_ref, rows_ref, sent_ref, planes_ref,
    picked_ref, picked_codes_ref, mine_codes_ref, masks_ref,
):
    users, group_rows, _ = rows_ref.shape
    picks = places_ref.shape[2]
    planes = planes_ref[...]
    lanes = lax.broadcasted_iota(jnp.int32, (picks, group_rows), 1)
    for user in range(users):
        places = places_ref[user]
        columns = jnp.transpose(jnp.broadcast_to(places, (picks, picks)))
        in_tail = (columns == lanes[:, :HALO]).astype(jnp.float32)
        masks_ref[user, 0:1] = ((places >= HALO) & (places < HALO + group_rows)).astype(jnp.float32)
        masks_ref[user, 1:2] = jnp.max(in_tail, axis=0, keepdims=True)
        wide = jnp.concatenate([columns - HALO] * (group_rows // picks), axis=1)
        chosen = (wide == lanes).astype(jnp.float32).astype(jnp.bfloat16)
        picked = jnp.dot(chosen, rows_ref[user], preferred_element_type=jnp.float32).astype(
            jnp.bfloat16
        )
        picked_ref[user] = picked
        picked_codes_ref[user] = soft_codes(picked, planes)
        mine_codes_ref[user] = soft_codes(sent_ref[user, HALO:], planes)


def attend_kernel(
    masks_ref, picked_ref, picked_codes_ref, sent_ref, mine_codes_ref, other_ref, planes_ref,
    part_ref,
):
    user_count, _, width = picked_ref.shape
    users = range(user_count)
    code_bits = planes_ref.shape[0]
    planes = planes_ref[...]
    codes = [soft_codes(other_ref[user], planes) for user in users]
    rows, similar = [], []
    for user in users:
        queries = jnp.concatenate([sent_ref[user, HALO:], other_ref[user, HALO:]], axis=0)
        rows.append(jnp.concatenate([picked_ref[user], other_ref[user, :HALO]], axis=0))
        similar.append(last_with_last(queries, rows[user]) * (1.0 / math.sqrt(width)))
    scores, usable = [], []
    for user in users:
        query_codes = jnp.concatenate([mine_codes_ref[user], codes[user][HALO:]], axis=0)
        row_codes = jnp.concatenate([picked_codes_ref[user], codes[user][:HALO]], axis=0)
        agreement = last_with_last(query_codes, row_codes)
        scores.append(similar[user] + HASH_WEIGHT / code_bits * agreement)
        usable.append(
            jnp.concatenate([masks_ref[user, 0:1], masks_ref[user, 1:2]], axis=1) > 0.0
        )
    group_max = [
        jnp.max(jnp.where(usable[user], scores[user], NEG_FILL), axis=1, keepdims=True)
        for user in users
    ]
    weights = [
        jnp.where(usable[user], jnp.exp(scores[user] - group_max[user]), 0.0) for user in users
    ]
    for user in users:
        part_ref[user, :, :width] = jnp.dot(
            weights[user].astype(jnp.bfloat16), rows[user], preferred_element_type=jnp.float32
        )
    for user in users:
        group_total = jnp.sum(weights[user], axis=1, keepdims=True)
        side_lane = lax.broadcasted_iota(jnp.int32, (group_total.shape[0], SIDE), 1)
        part_ref[user, :, width:] = jnp.where(
            side_lane < SIDE // 2, group_max[user], group_total
        )


def merge_kernel(mine_ref, other_ref, own_ref, moments_ref):
    users, cands, packed = mine_ref.shape
    width = packed - SIDE
    half = cands // 2
    low = lax.broadcasted_iota(jnp.int32, (half, SIDE), 1) < SIDE // 2
    sums, squares = [], []
    for user in range(users):
        for first in (0, half):
            here = (user, slice(first, first + half))
            there = (user, slice(half - first, cands - first))
            tops, totals = [], []
            for ref, at in ((mine_ref, here), (other_ref, there)):
                side = ref[at[0], at[1], width:]
                turned = pltpu.roll(side, SIDE // 2, 1)
                tops.append(jnp.where(low, side, turned))
                totals.append(jnp.where(low, turned, side))
            joint_max = jnp.maximum(*tops)
            scales = [jnp.exp(top - joint_max) for top in tops]
            denominator = scales[0] * totals[0] + scales[1] * totals[1]
            for column in range(0, width, SIDE):
                lanes = slice(column, column + SIDE)
                numerator = (
                    scales[0] * mine_ref[here[0], here[1], lanes]
                    + scales[1] * other_ref[there[0], there[1], lanes]
                )
                attended = numerator / denominator
                sums.append((column, jnp.sum(attended, axis=0, keepdims=True)))
                squares.append((column, jnp.sum(attended * attended, axis=0, keepdims=True)))
                if first == 0:
                    own_ref[user, :, lanes] = attended
    for row, terms in enumerate((sums, squares)):
        for column in range(0, width, SIDE):
            moments_ref[row : row + 1, column : column + SIDE] = sum(
                term for at, term in terms if at == column
            )


def two_groups(behaviors, candidates, ranks, lengths, hash_planes, norm_gain, norm_bias):
    users, group_rows, width = behaviors.shape
    own_cands = candidates.shape[1]
    picks = ranks.shape[2]
    cands = 2 * own_cands
    f32, bf16 = jnp.float32, jnp.bfloat16
    in_vmem = pl.BlockSpec(memory_space=pltpu.VMEM)
    swap = [(0, 1), (1, 0)]
    bits = hash_planes.shape[1]
    arguments = (ranks, lengths, norm_gain, norm_bias, hash_planes.T, candidates, behaviors)
    params = pltpu.CompilerParams(vmem_limit_bytes=VMEM_LIMIT)
    sent_bytes = 2 * users * (HALO + own_cands) * width
    sent, places, gain, bias, planes = pl.pallas_call(
        load_kernel,
        out_shape=(
            jax.ShapeDtypeStruct((users, HALO + own_cands, width), bf16),
            jax.ShapeDtypeStruct(ranks.shape, jnp.int32),
            jax.ShapeDtypeStruct(norm_gain.shape, f32),
            jax.ShapeDtypeStruct(norm_bias.shape, f32),
            jax.ShapeDtypeStruct((bits, width), bf16),
        ),
        in_specs=[pl.BlockSpec(memory_space=pl.ANY)] * len(arguments),
        out_specs=(in_vmem,) * 5,
        scratch_shapes=[
            pltpu.VMEM(ranks.shape, jnp.int32),
            pltpu.SMEM(lengths.shape, jnp.int32),
            pltpu.SemaphoreType.DMA((len(arguments),)),
        ],
        cost_estimate=pl.CostEstimate(flops=LOAD_COST, bytes_accessed=sent_bytes, transcendentals=0),
        compiler_params=params,
        name="load",
    )(*(pltpu.with_memory_space_constraint(value, pltpu.HBM) for value in arguments))
    other = lax.ppermute(sent, "seq", swap)
    picked, picked_codes, mine_codes, masks = pl.pallas_call(
        own_picks_kernel,
        out_shape=(
            jax.ShapeDtypeStruct((users, picks, width), bf16),
            jax.ShapeDtypeStruct((users, picks, bits), bf16),
            jax.ShapeDtypeStruct((users, own_cands, bits), bf16),
            jax.ShapeDtypeStruct((users, 2, picks), f32),
        ),
        in_specs=[in_vmem] * 4,
        out_specs=(in_vmem,) * 4,
        cost_estimate=pl.CostEstimate(
            flops=2 * users * picks * group_rows * width,
            bytes_accessed=behaviors.nbytes,
            transcendentals=0,
        ),
        compiler_params=params,
        name="own_picks",
    )(places, behaviors, sent, planes)
    part = pl.pallas_call(
        attend_kernel,
        out_shape=jax.ShapeDtypeStruct((users, cands, width + SIDE), f32),
        in_specs=[in_vmem] * 7,
        out_specs=in_vmem,
        compiler_params=params,
        name="attend",
    )(masks, picked, picked_codes, sent, mine_codes, other, planes)
    own, moments = pl.pallas_call(
        merge_kernel,
        out_shape=(
            jax.ShapeDtypeStruct((users, own_cands, width), f32),
            jax.ShapeDtypeStruct((2, width), f32),
        ),
        in_specs=[in_vmem] * 2,
        out_specs=(in_vmem,) * 2,
        compiler_params=params,
        name="merge",
    )(part, lax.ppermute(part, "seq", swap))
    row_count = users * cands * lax.axis_size("user")
    return normalized(own, user_total(moments), row_count, gain, bias)


def solution(mesh):
    in_specs = (
        P("user", "seq", None),
        P("user", "seq", None),
        P("user", "seq", None),
        P("user"),
        P(),
        P(),
        P(),
    )
    out_specs = P("user", "seq", None)
    shards = two_groups if mesh.shape["seq"] == 2 else any_groups
    return jax.shard_map(shards, mesh=mesh, in_specs=in_specs, out_specs=out_specs, check_vma=False)
```

```python
import math

import jax
import jax.numpy as jnp
from jax import lax
from jax.experimental import pallas as pl
from jax.experimental.pallas import tpu as pltpu
from jax.sharding import PartitionSpec as P

HALO = 128


NEG_FILL = -1e30
HASH_WEIGHT = 2.0
NORM_EPS = 1e-05

BOTH = ("user", "seq")
SIDE = 128
VMEM_LIMIT = 8 * 1024 * 1024
LOAD_COST = 10**8


def user_total(value):
    users, seqs = lax.axis_size("user"), lax.axis_size("seq")
    if users & (users - 1):
        return lax.psum(value, "user")
    stride = 1
    while stride < users:
        pairs = [
            (user * seqs + seq, (user ^ stride) * seqs + (seq ^ 1 if seqs % 2 == 0 else seq))
            for user in range(users)
            for seq in range(seqs)
        ]
        value = value + lax.ppermute(value, BOTH, pairs)
        stride *= 2
    return value


def last_with_last(left, right):
    return lax.dot_general(
        left, right, (((1,), (1,)), ((), ())), preferred_element_type=jnp.float32
    )


def soft_codes(rows, planes):
    return jnp.tanh(last_with_last(rows, planes)).astype(jnp.bfloat16)


def normalized(own, moments, row_count, norm_gain, norm_bias):
    feature_mean = moments[0] / row_count
    feature_var = moments[1] / row_count - feature_mean * feature_mean
    normed = (own - feature_mean) * lax.rsqrt(feature_var + NORM_EPS) * norm_gain + norm_bias
    return normed.astype(jnp.bfloat16)


def any_groups(behaviors, candidates, ranks, lengths, hash_planes, norm_gain, norm_bias):
    group_rows = behaviors.shape[1]
    feature_width = behaviors.shape[2]
    own_cands = candidates.shape[1]
    code_bits = hash_planes.shape[1]
    seqs = lax.axis_size("seq")
    seq_index = lax.axis_index("seq")
    tail_rows = behaviors[:, group_rows - HALO :, :]
    before = lax.ppermute(tail_rows, "seq", [(k, (k + 1) % seqs) for k in range(seqs)])
    queries = lax.all_gather(candidates, "seq", axis=1, tiled=True)
    window_pos = ranks[:, 0, :]
    from_tail = window_pos < HALO
    tail_index = jnp.clip(window_pos, 0, HALO - 1)
    own_index = jnp.clip(window_pos - HALO, 0, group_rows - 1)
    take_rows = jax.vmap(lambda row_table, where_at: row_table[where_at])
    picked = jnp.where(
        from_tail[:, :, None], take_rows(before, tail_index), take_rows(behaviors, own_index)
    )
    position = seq_index * group_rows - HALO + window_pos
    usable = (position >= 0) & (position < lengths[:, None])
    query_codes, picked_codes = (
        jnp.tanh(
            jnp.einsum("ukd,db->ukb", rows, hash_planes, preferred_element_type=jnp.float32)
        ).astype(jnp.bfloat16)
        for rows in (queries, picked)
    )
    similar = jnp.einsum("ucd,ukd->uck", queries, picked, preferred_element_type=jnp.float32)
    agreement = jnp.einsum(
        "ucb,ukb->uck", query_codes, picked_codes, preferred_element_type=jnp.float32
    )
    scores = similar * (1.0 / math.sqrt(feature_width)) + HASH_WEIGHT / code_bits * agreement
    usable_rows = usable[:, None, :]
    group_max = jnp.max(jnp.where(usable_rows, scores, NEG_FILL), axis=2)
    weights = jnp.where(usable_rows, jnp.exp(scores - group_max[..., None]), 0.0)
    group_total = jnp.sum(weights, axis=2)
    group_sum = jnp.einsum(
        "uck,ukd->ucd", weights.astype(jnp.bfloat16), picked, preferred_element_type=jnp.float32
    )
    tops = lax.all_gather(group_max, "seq")
    rescales = jnp.exp(tops - jnp.max(tops, axis=0))
    numerator = jnp.sum(rescales[..., None] * lax.all_gather(group_sum, "seq"), axis=0)
    denominator = jnp.sum(rescales * lax.all_gather(group_total, "seq"), axis=0)
    attended = numerator / denominator[..., None]
    moments = user_total(
        jnp.stack([jnp.sum(attended, axis=(0, 1)), jnp.sum(attended * attended, axis=(0, 1))])
    )
    row_count = attended.shape[0] * attended.shape[1] * lax.axis_size("user")
    own = lax.dynamic_slice_in_dim(attended, seq_index * own_cands, own_cands, 1)
    return normalized(own, moments, row_count, norm_gain, norm_bias)


def load_kernel(
    ranks_hbm, lengths_hbm, norm_gain_hbm, norm_bias_hbm, planes_hbm, mine_hbm, behaviors_hbm,
    sent_ref, places_ref, gain_ref, bias_ref, planes_ref,
    ranks, lengths, sems,
):
    users, group_rows, _ = behaviors_hbm.shape
    tail = group_rows - HALO
    pairs = [
        *(
            (behaviors_hbm.at[user, pl.ds(tail, HALO)], sent_ref.at[user, pl.ds(0, HALO)])
            for user in range(users)
        ),
        (mine_hbm, sent_ref.at[:, pl.ds(HALO, mine_hbm.shape[1])]),
        (ranks_hbm, ranks),
        (lengths_hbm, lengths),
        (planes_hbm, planes_ref),
        (norm_gain_hbm, gain_ref),
        (norm_bias_hbm, bias_ref),
    ]
    copies = [
        pltpu.make_async_copy(source, target, sems.at[k])
        for k, (source, target) in enumerate(pairs)
    ]
    for copy in copies:
        copy.start()
    for copy in copies[users + 1 : users + 3]:
        copy.wait()
    start = lax.axis_index("seq") * group_rows - HALO
    for user in range(users):
        position = ranks[user] + start
        usable = (position >= 0) & (position < lengths[user])
        places_ref[user] = jnp.where(usable, ranks[user], HALO + group_rows)
    for copy in copies[: users + 1] + copies[users + 3 :]:
        copy.wait()


def own_picks_kernel(
    places_ref, rows_ref, sent_ref, planes_ref,
    picked_ref, picked_codes_ref, mine_codes_ref, masks_ref,
):
    users, group_rows, _ = rows_ref.shape
    picks = places_ref.shape[2]
    planes = planes_ref[...]
    lanes = lax.broadcasted_iota(jnp.int32, (picks, group_rows), 1)
    for user in range(users):
        places = places_ref[user]
        columns = jnp.transpose(jnp.broadcast_to(places, (picks, picks)))
        in_tail = (columns == lanes[:, :HALO]).astype(jnp.float32)
        masks_ref[user, 0:1] = ((places >= HALO) & (places < HALO + group_rows)).astype(jnp.float32)
        masks_ref[user, 1:2] = jnp.max(in_tail, axis=0, keepdims=True)
        wide = jnp.concatenate([columns - HALO] * (group_rows // picks), axis=1)
        chosen = (wide == lanes).astype(jnp.float32).astype(jnp.bfloat16)
        picked = jnp.dot(chosen, rows_ref[user], preferred_element_type=jnp.float32).astype(
            jnp.bfloat16
        )
        picked_ref[user] = picked
        picked_codes_ref[user] = soft_codes(picked, planes)
        mine_codes_ref[user] = soft_codes(sent_ref[user, HALO:], planes)


def attend_kernel(
    masks_ref, picked_ref, picked_codes_ref, sent_ref, mine_codes_ref, other_ref, planes_ref,
    part_ref,
):
    user_count, _, width = picked_ref.shape
    users = range(user_count)
    code_bits = planes_ref.shape[0]
    planes = planes_ref[...]
    codes = [soft_codes(other_ref[user], planes) for user in users]
    rows, similar = [], []
    for user in users:
        queries = jnp.concatenate([sent_ref[user, HALO:], other_ref[user, HALO:]], axis=0)
        rows.append(jnp.concatenate([picked_ref[user], other_ref[user, :HALO]], axis=0))
        similar.append(last_with_last(queries, rows[user]) * (1.0 / math.sqrt(width)))
    scores, usable = [], []
    for user in users:
        query_codes = jnp.concatenate([mine_codes_ref[user], codes[user][HALO:]], axis=0)
        row_codes = jnp.concatenate([picked_codes_ref[user], codes[user][:HALO]], axis=0)
        agreement = last_with_last(query_codes, row_codes)
        scores.append(similar[user] + HASH_WEIGHT / code_bits * agreement)
        usable.append(
            jnp.concatenate([masks_ref[user, 0:1], masks_ref[user, 1:2]], axis=1) > 0.0
        )
    group_max = [
        jnp.max(jnp.where(usable[user], scores[user], NEG_FILL), axis=1, keepdims=True)
        for user in users
    ]
    weights = [
        jnp.where(usable[user], jnp.exp(scores[user] - group_max[user]), 0.0) for user in users
    ]
    for user in users:
        part_ref[user, :, :width] = jnp.dot(
            weights[user].astype(jnp.bfloat16), rows[user], preferred_element_type=jnp.float32
        )
    for user in users:
        group_total = jnp.sum(weights[user], axis=1, keepdims=True)
        side_lane = lax.broadcasted_iota(jnp.int32, (group_total.shape[0], SIDE), 1)
        part_ref[user, :, width:] = jnp.where(
            side_lane < SIDE // 2, group_max[user], group_total
        )


def merge_kernel(mine_ref, other_ref, own_ref, moments_ref):
    users, cands, packed = mine_ref.shape
    width = packed - SIDE
    half = cands // 2
    low = lax.broadcasted_iota(jnp.int32, (half, SIDE), 1) < SIDE // 2
    sums, squares = [], []
    for user in range(users):
        for first in (0, half):
            here = (user, slice(first, first + half))
            there = (user, slice(half - first, cands - first))
            tops, totals = [], []
            for ref, at in ((mine_ref, here), (other_ref, there)):
                side = ref[at[0], at[1], width:]
                turned = pltpu.roll(side, SIDE // 2, 1)
                tops.append(jnp.where(low, side, turned))
                totals.append(jnp.where(low, turned, side))
            joint_max = jnp.maximum(*tops)
            scales = [jnp.exp(top - joint_max) for top in tops]
            denominator = scales[0] * totals[0] + scales[1] * totals[1]
            for column in range(0, width, SIDE):
                lanes = slice(column, column + SIDE)
                numerator = (
                    scales[0] * mine_ref[here[0], here[1], lanes]
                    + scales[1] * other_ref[there[0], there[1], lanes]
                )
                attended = numerator / denominator
                sums.append((column, jnp.sum(attended, axis=0, keepdims=True)))
                squares.append((column, jnp.sum(attended * attended, axis=0, keepdims=True)))
                if first == 0:
                    own_ref[user, :, lanes] = attended
    for row, terms in enumerate((sums, squares)):
        for column in range(0, width, SIDE):
            moments_ref[row : row + 1, column : column + SIDE] = sum(
                term for at, term in terms if at == column
            )


def two_groups(behaviors, candidates, ranks, lengths, hash_planes, norm_gain, norm_bias):
    users, group_rows, width = behaviors.shape
    own_cands = candidates.shape[1]
    picks = ranks.shape[2]
    cands = 2 * own_cands
    f32, bf16 = jnp.float32, jnp.bfloat16
    in_vmem = pl.BlockSpec(memory_space=pltpu.VMEM)
    swap = [(0, 1), (1, 0)]
    bits = hash_planes.shape[1]
    arguments = (ranks, lengths, norm_gain, norm_bias, hash_planes.T, candidates, behaviors)
    params = pltpu.CompilerParams(vmem_limit_bytes=VMEM_LIMIT)
    sent_bytes = 2 * users * (HALO + own_cands) * width
    sent, places, gain, bias, planes = pl.pallas_call(
        load_kernel,
        out_shape=(
            jax.ShapeDtypeStruct((users, HALO + own_cands, width), bf16),
            jax.ShapeDtypeStruct(ranks.shape, jnp.int32),
            jax.ShapeDtypeStruct(norm_gain.shape, f32),
            jax.ShapeDtypeStruct(norm_bias.shape, f32),
            jax.ShapeDtypeStruct((bits, width), bf16),
        ),
        in_specs=[pl.BlockSpec(memory_space=pl.ANY)] * len(arguments),
        out_specs=(in_vmem,) * 5,
        scratch_shapes=[
            pltpu.VMEM(ranks.shape, jnp.int32),
            pltpu.SMEM(lengths.shape, jnp.int32),
            pltpu.SemaphoreType.DMA((len(arguments) + users - 1,)),
        ],
        cost_estimate=pl.CostEstimate(flops=LOAD_COST, bytes_accessed=sent_bytes, transcendentals=0),
        compiler_params=params,
        name="load",
    )(*(pltpu.with_memory_space_constraint(value, pltpu.HBM) for value in arguments))
    other = lax.ppermute(sent, "seq", swap)
    picked, picked_codes, mine_codes, masks = pl.pallas_call(
        own_picks_kernel,
        out_shape=(
            jax.ShapeDtypeStruct((users, picks, width), bf16),
            jax.ShapeDtypeStruct((users, picks, bits), bf16),
            jax.ShapeDtypeStruct((users, own_cands, bits), bf16),
            jax.ShapeDtypeStruct((users, 2, picks), f32),
        ),
        in_specs=[in_vmem] * 4,
        out_specs=(in_vmem,) * 4,
        cost_estimate=pl.CostEstimate(
            flops=2 * users * picks * group_rows * width,
            bytes_accessed=behaviors.nbytes,
            transcendentals=0,
        ),
        compiler_params=params,
        name="own_picks",
    )(places, behaviors, sent, planes)
    part = pl.pallas_call(
        attend_kernel,
        out_shape=jax.ShapeDtypeStruct((users, cands, width + SIDE), f32),
        in_specs=[in_vmem] * 7,
        out_specs=in_vmem,
        compiler_params=params,
        name="attend",
    )(masks, picked, picked_codes, sent, mine_codes, other, planes)
    own, moments = pl.pallas_call(
        merge_kernel,
        out_shape=(
            jax.ShapeDtypeStruct((users, own_cands, width), f32),
            jax.ShapeDtypeStruct((2, width), f32),
        ),
        in_specs=[in_vmem] * 2,
        out_specs=(in_vmem,) * 2,
        compiler_params=params,
        name="merge",
    )(part, lax.ppermute(part, "seq", swap))
    row_count = users * cands * lax.axis_size("user")
    return normalized(own, user_total(moments), row_count, gain, bias)


def solution(mesh):
    in_specs = (
        P("user", "seq", None),
        P("user", "seq", None),
        P("user", "seq", None),
        P("user"),
        P(),
        P(),
        P(),
    )
    out_specs = P("user", "seq", None)
    shards = two_groups if mesh.shape["seq"] == 2 else any_groups
    return jax.shard_map(shards, mesh=mesh, in_specs=in_specs, out_specs=out_specs, check_vma=False)
```

```python
import math

import jax
import jax.numpy as jnp
from jax import lax
from jax.experimental import pallas as pl
from jax.experimental.pallas import tpu as pltpu
from jax.sharding import PartitionSpec as P

HALO = 128


NEG_FILL = -1e30
HASH_WEIGHT = 2.0
NORM_EPS = 1e-05

BOTH = ("user", "seq")
SIDE = 128
VMEM_LIMIT = 8 * 1024 * 1024
LOAD_COST = 10**8


def user_total(value):
    users, seqs = lax.axis_size("user"), lax.axis_size("seq")
    if users & (users - 1):
        return lax.psum(value, "user")
    stride = 1
    while stride < users:
        pairs = [
            (user * seqs + seq, (user ^ stride) * seqs + (seq ^ 1 if seqs % 2 == 0 else seq))
            for user in range(users)
            for seq in range(seqs)
        ]
        value = value + lax.ppermute(value, BOTH, pairs)
        stride *= 2
    return value


def last_with_last(left, right):
    return lax.dot_general(
        left, right, (((1,), (1,)), ((), ())), preferred_element_type=jnp.float32
    )


def soft_codes(rows, planes):
    return jnp.tanh(last_with_last(rows, planes)).astype(jnp.bfloat16)


def normalized(own, moments, row_count, norm_gain, norm_bias):
    feature_mean = moments[0] / row_count
    feature_var = moments[1] / row_count - feature_mean * feature_mean
    normed = (own - feature_mean) * lax.rsqrt(feature_var + NORM_EPS) * norm_gain + norm_bias
    return normed.astype(jnp.bfloat16)


def any_groups(behaviors, candidates, ranks, lengths, hash_planes, norm_gain, norm_bias):
    group_rows = behaviors.shape[1]
    feature_width = behaviors.shape[2]
    own_cands = candidates.shape[1]
    code_bits = hash_planes.shape[1]
    seqs = lax.axis_size("seq")
    seq_index = lax.axis_index("seq")
    tail_rows = behaviors[:, group_rows - HALO :, :]
    before = lax.ppermute(tail_rows, "seq", [(k, (k + 1) % seqs) for k in range(seqs)])
    queries = lax.all_gather(candidates, "seq", axis=1, tiled=True)
    window_pos = ranks[:, 0, :]
    from_tail = window_pos < HALO
    tail_index = jnp.clip(window_pos, 0, HALO - 1)
    own_index = jnp.clip(window_pos - HALO, 0, group_rows - 1)
    take_rows = jax.vmap(lambda row_table, where_at: row_table[where_at])
    picked = jnp.where(
        from_tail[:, :, None], take_rows(before, tail_index), take_rows(behaviors, own_index)
    )
    position = seq_index * group_rows - HALO + window_pos
    usable = (position >= 0) & (position < lengths[:, None])
    query_codes, picked_codes = (
        jnp.tanh(
            jnp.einsum("ukd,db->ukb", rows, hash_planes, preferred_element_type=jnp.float32)
        ).astype(jnp.bfloat16)
        for rows in (queries, picked)
    )
    similar = jnp.einsum("ucd,ukd->uck", queries, picked, preferred_element_type=jnp.float32)
    agreement = jnp.einsum(
        "ucb,ukb->uck", query_codes, picked_codes, preferred_element_type=jnp.float32
    )
    scores = similar * (1.0 / math.sqrt(feature_width)) + HASH_WEIGHT / code_bits * agreement
    usable_rows = usable[:, None, :]
    group_max = jnp.max(jnp.where(usable_rows, scores, NEG_FILL), axis=2)
    weights = jnp.where(usable_rows, jnp.exp(scores - group_max[..., None]), 0.0)
    group_total = jnp.sum(weights, axis=2)
    group_sum = jnp.einsum(
        "uck,ukd->ucd", weights.astype(jnp.bfloat16), picked, preferred_element_type=jnp.float32
    )
    tops = lax.all_gather(group_max, "seq")
    rescales = jnp.exp(tops - jnp.max(tops, axis=0))
    numerator = jnp.sum(rescales[..., None] * lax.all_gather(group_sum, "seq"), axis=0)
    denominator = jnp.sum(rescales * lax.all_gather(group_total, "seq"), axis=0)
    attended = numerator / denominator[..., None]
    moments = user_total(
        jnp.stack([jnp.sum(attended, axis=(0, 1)), jnp.sum(attended * attended, axis=(0, 1))])
    )
    row_count = attended.shape[0] * attended.shape[1] * lax.axis_size("user")
    own = lax.dynamic_slice_in_dim(attended, seq_index * own_cands, own_cands, 1)
    return normalized(own, moments, row_count, norm_gain, norm_bias)


def load_kernel(
    ranks_hbm, lengths_hbm, norm_gain_hbm, norm_bias_hbm, planes_hbm, mine_hbm, behaviors_hbm,
    sent_ref, places_ref, gain_ref, bias_ref, planes_ref,
    ranks, lengths, sems,
):
    users, group_rows, _ = behaviors_hbm.shape
    tail = group_rows - HALO
    pairs = [
        *(
            (behaviors_hbm.at[user, pl.ds(tail, HALO)], sent_ref.at[user, pl.ds(0, HALO)])
            for user in range(users)
        ),
        (mine_hbm, sent_ref.at[:, pl.ds(HALO, mine_hbm.shape[1])]),
        (ranks_hbm, ranks),
        (lengths_hbm, lengths),
        (planes_hbm, planes_ref),
        (norm_gain_hbm, gain_ref),
        (norm_bias_hbm, bias_ref),
    ]
    copies = [
        pltpu.make_async_copy(source, target, sems.at[k])
        for k, (source, target) in enumerate(pairs)
    ]
    for copy in copies:
        copy.start()
    for copy in copies[users + 1 : users + 3]:
        copy.wait()
    start = lax.axis_index("seq") * group_rows - HALO
    for user in range(users):
        position = ranks[user] + start
        usable = (position >= 0) & (position < lengths[user])
        places_ref[user] = jnp.where(usable, ranks[user], HALO + group_rows)
    for copy in copies[: users + 1] + copies[users + 3 :]:
        copy.wait()


def own_picks_kernel(
    places_ref, rows_ref, sent_ref, planes_ref,
    picked_ref, picked_codes_ref, mine_codes_ref, masks_ref,
):
    users, group_rows, _ = rows_ref.shape
    picks = places_ref.shape[2]
    planes = planes_ref[...]
    lanes = lax.broadcasted_iota(jnp.int32, (picks, group_rows), 1)
    for user in range(users):
        places = places_ref[user]
        columns = jnp.transpose(jnp.broadcast_to(places, (picks, picks)))
        in_tail = (columns == lanes[:, :HALO]).astype(jnp.float32)
        masks_ref[user, 0:1] = ((places >= HALO) & (places < HALO + group_rows)).astype(jnp.float32)
        masks_ref[user, 1:2] = jnp.max(in_tail, axis=0, keepdims=True)
        wide = jnp.concatenate([columns - HALO] * (group_rows // picks), axis=1)
        chosen = (wide == lanes).astype(jnp.float32).astype(jnp.bfloat16)
        picked = jnp.dot(chosen, rows_ref[user], preferred_element_type=jnp.float32).astype(
            jnp.bfloat16
        )
        picked_ref[user] = picked
        picked_codes_ref[user] = soft_codes(picked, planes)
        mine_codes_ref[user] = soft_codes(sent_ref[user, HALO:], planes)


def attend_kernel(
    masks_ref, picked_ref, picked_codes_ref, sent_ref, mine_codes_ref, other_ref, planes_ref,
    part_ref,
):
    user_count, _, width = picked_ref.shape
    users = range(user_count)
    code_bits = planes_ref.shape[0]
    planes = planes_ref[...]
    codes = [soft_codes(other_ref[user], planes) for user in users]
    rows, similar = [], []
    for user in users:
        queries = jnp.concatenate([sent_ref[user, HALO:], other_ref[user, HALO:]], axis=0)
        rows.append(jnp.concatenate([picked_ref[user], other_ref[user, :HALO]], axis=0))
        similar.append(last_with_last(queries, rows[user]) * (1.0 / math.sqrt(width)))
    scores, usable = [], []
    for user in users:
        query_codes = jnp.concatenate([mine_codes_ref[user], codes[user][HALO:]], axis=0)
        row_codes = jnp.concatenate([picked_codes_ref[user], codes[user][:HALO]], axis=0)
        agreement = last_with_last(query_codes, row_codes)
        scores.append(similar[user] + HASH_WEIGHT / code_bits * agreement)
        usable.append(
            jnp.concatenate([masks_ref[user, 0:1], masks_ref[user, 1:2]], axis=1) > 0.0
        )
    group_max = [
        jnp.max(jnp.where(usable[user], scores[user], NEG_FILL), axis=1, keepdims=True)
        for user in users
    ]
    weights = [
        jnp.where(usable[user], jnp.exp(scores[user] - group_max[user]), 0.0) for user in users
    ]
    for user in users:
        part_ref[user, :, :width] = jnp.dot(
            weights[user].astype(jnp.bfloat16), rows[user], preferred_element_type=jnp.float32
        )
    for user in users:
        group_total = jnp.sum(weights[user], axis=1, keepdims=True)
        side_lane = lax.broadcasted_iota(jnp.int32, (group_total.shape[0], SIDE), 1)
        part_ref[user, :, width:] = jnp.where(
            side_lane < SIDE // 2, group_max[user], group_total
        )


def merge_kernel(mine_ref, other_ref, own_ref, moments_ref):
    users, cands, packed = mine_ref.shape
    width = packed - SIDE
    half = cands // 2
    low = lax.broadcasted_iota(jnp.int32, (half, SIDE), 1) < SIDE // 2
    sums, squares = [], []
    for user in range(users):
        for first in (0, half):
            here = (user, slice(first, first + half))
            there = (user, slice(half - first, cands - first))
            tops, totals = [], []
            for ref, at in ((mine_ref, here), (other_ref, there)):
                side = ref[at[0], at[1], width:]
                turned = pltpu.roll(side, SIDE // 2, 1)
                tops.append(jnp.where(low, side, turned))
                totals.append(jnp.where(low, turned, side))
            joint_max = jnp.maximum(*tops)
            scales = [jnp.exp(top - joint_max) for top in tops]
            denominator = scales[0] * totals[0] + scales[1] * totals[1]
            for column in range(0, width, SIDE):
                lanes = slice(column, column + SIDE)
                numerator = (
                    scales[0] * mine_ref[here[0], here[1], lanes]
                    + scales[1] * other_ref[there[0], there[1], lanes]
                )
                attended = numerator / denominator
                sums.append((column, jnp.sum(attended, axis=0, keepdims=True)))
                squares.append((column, jnp.sum(attended * attended, axis=0, keepdims=True)))
                if first == 0:
                    own_ref[user, :, lanes] = attended
    for row, terms in enumerate((sums, squares)):
        for column in range(0, width, SIDE):
            moments_ref[row : row + 1, column : column + SIDE] = sum(
                term for at, term in terms if at == column
            )


def two_groups(behaviors, candidates, ranks, lengths, hash_planes, norm_gain, norm_bias):
    users, group_rows, width = behaviors.shape
    own_cands = candidates.shape[1]
    picks = ranks.shape[2]
    cands = 2 * own_cands
    f32, bf16 = jnp.float32, jnp.bfloat16
    in_vmem = pl.BlockSpec(memory_space=pltpu.VMEM)
    swap = [(0, 1), (1, 0)]
    bits = hash_planes.shape[1]
    arguments = (ranks, lengths, norm_gain, norm_bias, hash_planes.T, candidates, behaviors)
    params = pltpu.CompilerParams(vmem_limit_bytes=VMEM_LIMIT)
    scheduled = pltpu.CompilerParams(
        vmem_limit_bytes=VMEM_LIMIT
    )
    sent_bytes = 2 * users * (HALO + own_cands) * width
    sent, places, gain, bias, planes = pl.pallas_call(
        load_kernel,
        out_shape=(
            jax.ShapeDtypeStruct((users, HALO + own_cands, width), bf16),
            jax.ShapeDtypeStruct(ranks.shape, jnp.int32),
            jax.ShapeDtypeStruct(norm_gain.shape, f32),
            jax.ShapeDtypeStruct(norm_bias.shape, f32),
            jax.ShapeDtypeStruct((bits, width), bf16),
        ),
        in_specs=[pl.BlockSpec(memory_space=pl.ANY)] * len(arguments),
        out_specs=(in_vmem,) * 5,
        scratch_shapes=[
            pltpu.VMEM(ranks.shape, jnp.int32),
            pltpu.SMEM(lengths.shape, jnp.int32),
            pltpu.SemaphoreType.DMA((len(arguments) + users - 1,)),
        ],
        cost_estimate=pl.CostEstimate(flops=LOAD_COST, bytes_accessed=sent_bytes, transcendentals=0),
        compiler_params=params,
        name="load",
    )(*(pltpu.with_memory_space_constraint(value, pltpu.HBM) for value in arguments))
    other = lax.ppermute(sent, "seq", swap)
    picked, picked_codes, mine_codes, masks = pl.pallas_call(
        own_picks_kernel,
        out_shape=(
            jax.ShapeDtypeStruct((users, picks, width), bf16),
            jax.ShapeDtypeStruct((users, picks, bits), bf16),
            jax.ShapeDtypeStruct((users, own_cands, bits), bf16),
            jax.ShapeDtypeStruct((users, 2, picks), f32),
        ),
        in_specs=[in_vmem] * 4,
        out_specs=(in_vmem,) * 4,
        cost_estimate=pl.CostEstimate(
            flops=2 * users * picks * group_rows * width,
            bytes_accessed=behaviors.nbytes,
            transcendentals=0,
        ),
        compiler_params=scheduled,
        name="own_picks",
    )(places, behaviors, sent, planes)
    part = pl.pallas_call(
        attend_kernel,
        out_shape=jax.ShapeDtypeStruct((users, cands, width + SIDE), f32),
        in_specs=[in_vmem] * 7,
        out_specs=in_vmem,
        compiler_params=scheduled,
        name="attend",
    )(masks, picked, picked_codes, sent, mine_codes, other, planes)
    own, moments = pl.pallas_call(
        merge_kernel,
        out_shape=(
            jax.ShapeDtypeStruct((users, own_cands, width), f32),
            jax.ShapeDtypeStruct((2, width), f32),
        ),
        in_specs=[in_vmem] * 2,
        out_specs=(in_vmem,) * 2,
        compiler_params=scheduled,
        name="merge",
    )(part, lax.ppermute(part, "seq", swap))
    row_count = users * cands * lax.axis_size("user")
    return normalized(own, user_total(moments), row_count, gain, bias)


def solution(mesh):
    in_specs = (
        P("user", "seq", None),
        P("user", "seq", None),
        P("user", "seq", None),
        P("user"),
        P(),
        P(),
        P(),
    )
    out_specs = P("user", "seq", None)
    shards = two_groups if mesh.shape["seq"] == 2 else any_groups
    return jax.shard_map(shards, mesh=mesh, in_specs=in_specs, out_specs=out_specs, check_vma=False)
```

```python
import functools
import math

import jax
import jax.numpy as jnp
from jax import lax
from jax.experimental import pallas as pl
from jax.experimental.pallas import tpu as pltpu
from jax.sharding import PartitionSpec as P

HALO = 128


NEG_FILL = -1e30
HASH_WEIGHT = 2.0
NORM_EPS = 1e-05

BOTH = ("user", "seq")
SIDE = 128
VMEM_LIMIT = 8 * 1024 * 1024
LOAD_COST = 10**8


def user_total(value):
    users, seqs = lax.axis_size("user"), lax.axis_size("seq")
    if users & (users - 1):
        return lax.psum(value, "user")
    stride = 1
    while stride < users:
        pairs = [
            (user * seqs + seq, (user ^ stride) * seqs + (seq ^ 1 if seqs % 2 == 0 else seq))
            for user in range(users)
            for seq in range(seqs)
        ]
        value = value + lax.ppermute(value, BOTH, pairs)
        stride *= 2
    return value


def last_with_last(left, right):
    return lax.dot_general(
        left, right, (((1,), (1,)), ((), ())), preferred_element_type=jnp.float32
    )


def soft_codes(rows, planes):
    return jnp.tanh(last_with_last(rows, planes)).astype(jnp.bfloat16)


def normalized(own, moments, row_count, norm_gain, norm_bias):
    feature_mean = moments[0] / row_count
    feature_var = moments[1] / row_count - feature_mean * feature_mean
    normed = (own - feature_mean) * lax.rsqrt(feature_var + NORM_EPS) * norm_gain + norm_bias
    return normed.astype(jnp.bfloat16)


def any_groups(behaviors, candidates, ranks, lengths, hash_planes, norm_gain, norm_bias):
    group_rows = behaviors.shape[1]
    feature_width = behaviors.shape[2]
    own_cands = candidates.shape[1]
    code_bits = hash_planes.shape[1]
    seqs = lax.axis_size("seq")
    seq_index = lax.axis_index("seq")
    tail_rows = behaviors[:, group_rows - HALO :, :]
    before = lax.ppermute(tail_rows, "seq", [(k, (k + 1) % seqs) for k in range(seqs)])
    queries = lax.all_gather(candidates, "seq", axis=1, tiled=True)
    window_pos = ranks[:, 0, :]
    from_tail = window_pos < HALO
    tail_index = jnp.clip(window_pos, 0, HALO - 1)
    own_index = jnp.clip(window_pos - HALO, 0, group_rows - 1)
    take_rows = jax.vmap(lambda row_table, where_at: row_table[where_at])
    picked = jnp.where(
        from_tail[:, :, None], take_rows(before, tail_index), take_rows(behaviors, own_index)
    )
    position = seq_index * group_rows - HALO + window_pos
    usable = (position >= 0) & (position < lengths[:, None])
    query_codes, picked_codes = (
        jnp.tanh(
            jnp.einsum("ukd,db->ukb", rows, hash_planes, preferred_element_type=jnp.float32)
        ).astype(jnp.bfloat16)
        for rows in (queries, picked)
    )
    similar = jnp.einsum("ucd,ukd->uck", queries, picked, preferred_element_type=jnp.float32)
    agreement = jnp.einsum(
        "ucb,ukb->uck", query_codes, picked_codes, preferred_element_type=jnp.float32
    )
    scores = similar * (1.0 / math.sqrt(feature_width)) + HASH_WEIGHT / code_bits * agreement
    usable_rows = usable[:, None, :]
    group_max = jnp.max(jnp.where(usable_rows, scores, NEG_FILL), axis=2)
    weights = jnp.where(usable_rows, jnp.exp(scores - group_max[..., None]), 0.0)
    group_total = jnp.sum(weights, axis=2)
    group_sum = jnp.einsum(
        "uck,ukd->ucd", weights.astype(jnp.bfloat16), picked, preferred_element_type=jnp.float32
    )
    tops = lax.all_gather(group_max, "seq")
    rescales = jnp.exp(tops - jnp.max(tops, axis=0))
    numerator = jnp.sum(rescales[..., None] * lax.all_gather(group_sum, "seq"), axis=0)
    denominator = jnp.sum(rescales * lax.all_gather(group_total, "seq"), axis=0)
    attended = numerator / denominator[..., None]
    moments = user_total(
        jnp.stack([jnp.sum(attended, axis=(0, 1)), jnp.sum(attended * attended, axis=(0, 1))])
    )
    row_count = attended.shape[0] * attended.shape[1] * lax.axis_size("user")
    own = lax.dynamic_slice_in_dim(attended, seq_index * own_cands, own_cands, 1)
    return normalized(own, moments, row_count, norm_gain, norm_bias)


def load_kernel(
    ranks_hbm, lengths_hbm, norm_gain_hbm, norm_bias_hbm, planes_hbm, mine_hbm, behaviors_hbm,
    sent_ref, places_ref, gain_ref, bias_ref, planes_ref,
    ranks, lengths, sems,
):
    users, group_rows, _ = behaviors_hbm.shape
    tail = group_rows - HALO
    pairs = [
        *(
            (behaviors_hbm.at[user, pl.ds(tail, HALO)], sent_ref.at[user, pl.ds(0, HALO)])
            for user in range(users)
        ),
        (mine_hbm, sent_ref.at[:, pl.ds(HALO, mine_hbm.shape[1])]),
        (ranks_hbm, ranks),
        (lengths_hbm, lengths),
        (planes_hbm, planes_ref),
        (norm_gain_hbm, gain_ref),
        (norm_bias_hbm, bias_ref),
    ]
    copies = [
        pltpu.make_async_copy(source, target, sems.at[k])
        for k, (source, target) in enumerate(pairs)
    ]
    for copy in copies:
        copy.start()
    for copy in copies[users + 1 : users + 3]:
        copy.wait()
    start = lax.axis_index("seq") * group_rows - HALO
    for user in range(users):
        position = ranks[user] + start
        usable = (position >= 0) & (position < lengths[user])
        places_ref[user] = jnp.where(usable, ranks[user], HALO + group_rows)
    for copy in copies[: users + 1] + copies[users + 3 :]:
        copy.wait()


def own_picks_kernel(
    places_ref, rows_ref, sent_ref, planes_ref,
    picked_ref, picked_codes_ref, mine_codes_ref, masks_ref,
):
    users, group_rows, _ = rows_ref.shape
    picks = places_ref.shape[2]
    planes = planes_ref[...]
    lanes = lax.broadcasted_iota(jnp.int32, (picks, group_rows), 1)
    for user in range(users):
        places = places_ref[user]
        columns = jnp.transpose(jnp.broadcast_to(places, (picks, picks)))
        in_tail = (columns == lanes[:, :HALO]).astype(jnp.float32)
        masks_ref[user, 0:1] = ((places >= HALO) & (places < HALO + group_rows)).astype(jnp.float32)
        masks_ref[user, 1:2] = jnp.max(in_tail, axis=0, keepdims=True)
        wide = jnp.concatenate([columns - HALO] * (group_rows // picks), axis=1)
        chosen = (wide == lanes).astype(jnp.float32).astype(jnp.bfloat16)
        picked = jnp.dot(chosen, rows_ref[user], preferred_element_type=jnp.float32).astype(
            jnp.bfloat16
        )
        picked_ref[user] = picked
        picked_codes_ref[user] = soft_codes(picked, planes)
        mine_codes_ref[user] = soft_codes(sent_ref[user, HALO:], planes)


def attend_kernel(
    masks_ref, picked_ref, picked_codes_ref, sent_ref, mine_codes_ref, other_ref, planes_ref,
    part_ref,
):
    user_count, _, width = picked_ref.shape
    users = range(user_count)
    code_bits = planes_ref.shape[0]
    planes = planes_ref[...]
    codes = [soft_codes(other_ref[user], planes) for user in users]
    rows, similar = [], []
    for user in users:
        queries = jnp.concatenate([sent_ref[user, HALO:], other_ref[user, HALO:]], axis=0)
        rows.append(jnp.concatenate([picked_ref[user], other_ref[user, :HALO]], axis=0))
        similar.append(last_with_last(queries, rows[user]) * (1.0 / math.sqrt(width)))
    scores, usable = [], []
    for user in users:
        query_codes = jnp.concatenate([mine_codes_ref[user], codes[user][HALO:]], axis=0)
        row_codes = jnp.concatenate([picked_codes_ref[user], codes[user][:HALO]], axis=0)
        agreement = last_with_last(query_codes, row_codes)
        scores.append(similar[user] + HASH_WEIGHT / code_bits * agreement)
        usable.append(
            jnp.concatenate([masks_ref[user, 0:1], masks_ref[user, 1:2]], axis=1) > 0.0
        )
    group_max = [
        jnp.max(jnp.where(usable[user], scores[user], NEG_FILL), axis=1, keepdims=True)
        for user in users
    ]
    weights = [
        jnp.where(usable[user], jnp.exp(scores[user] - group_max[user]), 0.0) for user in users
    ]
    for user in users:
        part_ref[user, :, :width] = jnp.dot(
            weights[user].astype(jnp.bfloat16), rows[user], preferred_element_type=jnp.float32
        )
    for user in users:
        group_total = jnp.sum(weights[user], axis=1, keepdims=True)
        side_lane = lax.broadcasted_iota(jnp.int32, (group_total.shape[0], SIDE), 1)
        part_ref[user, :, width:] = jnp.where(
            side_lane < SIDE // 2, group_max[user], group_total
        )


def merge_kernel(mine_ref, other_ref, own_ref, moments_ref):
    users, cands, packed = mine_ref.shape
    width = packed - SIDE
    half = cands // 2
    low = lax.broadcasted_iota(jnp.int32, (half, SIDE), 1) < SIDE // 2
    sums, squares = [], []
    for user in range(users):
        for first in (0, half):
            here = (user, slice(first, first + half))
            there = (user, slice(half - first, cands - first))
            tops, totals = [], []
            for ref, at in ((mine_ref, here), (other_ref, there)):
                side = ref[at[0], at[1], width:]
                turned = pltpu.roll(side, SIDE // 2, 1)
                tops.append(jnp.where(low, side, turned))
                totals.append(jnp.where(low, turned, side))
            joint_max = jnp.maximum(*tops)
            scales = [jnp.exp(top - joint_max) for top in tops]
            denominator = scales[0] * totals[0] + scales[1] * totals[1]
            for column in range(0, width, SIDE):
                lanes = slice(column, column + SIDE)
                numerator = (
                    scales[0] * mine_ref[here[0], here[1], lanes]
                    + scales[1] * other_ref[there[0], there[1], lanes]
                )
                attended = numerator / denominator
                sums.append((column, jnp.sum(attended, axis=0, keepdims=True)))
                squares.append((column, jnp.sum(attended * attended, axis=0, keepdims=True)))
                if first == 0:
                    own_ref[user, :, lanes] = attended
    for row, terms in enumerate((sums, squares)):
        for column in range(0, width, SIDE):
            moments_ref[row : row + 1, column : column + SIDE] = sum(
                term for at, term in terms if at == column
            )


def normalize_kernel(row_count, own_ref, moments_ref, gain_ref, bias_ref, out_ref):
    feature_mean = moments_ref[0:1] / row_count
    feature_var = moments_ref[1:2] / row_count - feature_mean * feature_mean
    scale = lax.rsqrt(feature_var + NORM_EPS)
    for user in range(own_ref.shape[0]):
        normed = (own_ref[user] - feature_mean) * scale * gain_ref[...] + bias_ref[...]
        out_ref[user] = normed.astype(jnp.bfloat16)


def two_groups(behaviors, candidates, ranks, lengths, hash_planes, norm_gain, norm_bias):
    users, group_rows, width = behaviors.shape
    own_cands = candidates.shape[1]
    picks = ranks.shape[2]
    cands = 2 * own_cands
    f32, bf16 = jnp.float32, jnp.bfloat16
    in_vmem = pl.BlockSpec(memory_space=pltpu.VMEM)
    swap = [(0, 1), (1, 0)]
    bits = hash_planes.shape[1]
    arguments = (
        ranks,
        lengths,
        norm_gain.reshape(1, width),
        norm_bias.reshape(1, width),
        hash_planes.T,
        candidates,
        behaviors,
    )
    params = pltpu.CompilerParams(vmem_limit_bytes=VMEM_LIMIT)
    scheduled = pltpu.CompilerParams(
        vmem_limit_bytes=VMEM_LIMIT
    )
    sent_bytes = 2 * users * (HALO + own_cands) * width
    sent, places, gain, bias, planes = pl.pallas_call(
        load_kernel,
        out_shape=(
            jax.ShapeDtypeStruct((users, HALO + own_cands, width), bf16),
            jax.ShapeDtypeStruct(ranks.shape, jnp.int32),
            jax.ShapeDtypeStruct((1, width), f32),
            jax.ShapeDtypeStruct((1, width), f32),
            jax.ShapeDtypeStruct((bits, width), bf16),
        ),
        in_specs=[pl.BlockSpec(memory_space=pl.ANY)] * len(arguments),
        out_specs=(in_vmem,) * 5,
        scratch_shapes=[
            pltpu.VMEM(ranks.shape, jnp.int32),
            pltpu.SMEM(lengths.shape, jnp.int32),
            pltpu.SemaphoreType.DMA((len(arguments) + users - 1,)),
        ],
        cost_estimate=pl.CostEstimate(flops=LOAD_COST, bytes_accessed=sent_bytes, transcendentals=0),
        compiler_params=params,
        name="load",
    )(*(pltpu.with_memory_space_constraint(value, pltpu.HBM) for value in arguments))
    other = lax.ppermute(sent, "seq", swap)
    picked, picked_codes, mine_codes, masks = pl.pallas_call(
        own_picks_kernel,
        out_shape=(
            jax.ShapeDtypeStruct((users, picks, width), bf16),
            jax.ShapeDtypeStruct((users, picks, bits), bf16),
            jax.ShapeDtypeStruct((users, own_cands, bits), bf16),
            jax.ShapeDtypeStruct((users, 2, picks), f32),
        ),
        in_specs=[in_vmem] * 4,
        out_specs=(in_vmem,) * 4,
        cost_estimate=pl.CostEstimate(
            flops=2 * users * picks * group_rows * width,
            bytes_accessed=behaviors.nbytes,
            transcendentals=0,
        ),
        compiler_params=scheduled,
        name="own_picks",
    )(places, behaviors, sent, planes)
    part = pl.pallas_call(
        attend_kernel,
        out_shape=jax.ShapeDtypeStruct((users, cands, width + SIDE), f32),
        in_specs=[in_vmem] * 7,
        out_specs=in_vmem,
        compiler_params=scheduled,
        name="attend",
    )(masks, picked, picked_codes, sent, mine_codes, other, planes)
    own, moments = pl.pallas_call(
        merge_kernel,
        out_shape=(
            jax.ShapeDtypeStruct((users, own_cands, width), f32),
            jax.ShapeDtypeStruct((2, width), f32),
        ),
        in_specs=[in_vmem] * 2,
        out_specs=(in_vmem,) * 2,
        compiler_params=scheduled,
        name="merge",
    )(part, lax.ppermute(part, "seq", swap))
    row_count = users * cands * lax.axis_size("user")
    return pl.pallas_call(
        functools.partial(normalize_kernel, row_count),
        out_shape=jax.ShapeDtypeStruct((users, own_cands, width), bf16),
        in_specs=[in_vmem] * 4,
        out_specs=in_vmem,
        compiler_params=params,
        name="normalize",
    )(own, user_total(moments), gain, bias)


def solution(mesh):
    in_specs = (
        P("user", "seq", None),
        P("user", "seq", None),
        P("user", "seq", None),
        P("user"),
        P(),
        P(),
        P(),
    )
    out_specs = P("user", "seq", None)
    shards = two_groups if mesh.shape["seq"] == 2 else any_groups
    return jax.shard_map(shards, mesh=mesh, in_specs=in_specs, out_specs=out_specs, check_vma=False)
```

```python
import math

import jax
import jax.numpy as jnp
from jax import lax
from jax.experimental import pallas as pl
from jax.experimental.pallas import tpu as pltpu
from jax.sharding import PartitionSpec as P

HALO = 128


NEG_FILL = -1e30
HASH_WEIGHT = 2.0
NORM_EPS = 1e-05

BOTH = ("user", "seq")
SIDE = 128
VMEM_LIMIT = 8 * 1024 * 1024
LOAD_COST = 10**8


def user_total(value):
    users, seqs = lax.axis_size("user"), lax.axis_size("seq")
    if users & (users - 1):
        return lax.psum(value, "user")
    stride = 1
    while stride < users:
        steps = (2, 3, 1) if stride == 1 and users >= 4 else (stride,)
        arrived = [
            lax.ppermute(
                value,
                BOTH,
                [
                    (user * seqs + seq, (user ^ step) * seqs + (seq ^ 1 if seqs % 2 == 0 else seq))
                    for user in range(users)
                    for seq in range(seqs)
                ],
            )
            for step in steps
        ]
        value = sum(arrived, value)
        stride *= 1 + len(steps)
    return value


def last_with_last(left, right):
    return lax.dot_general(
        left, right, (((1,), (1,)), ((), ())), preferred_element_type=jnp.float32
    )


def soft_codes(rows, planes):
    return jnp.tanh(last_with_last(rows, planes)).astype(jnp.bfloat16)


def normalized(own, moments, row_count, norm_gain, norm_bias):
    feature_mean = moments[0] / row_count
    feature_var = moments[1] / row_count - feature_mean * feature_mean
    normed = (own - feature_mean) * lax.rsqrt(feature_var + NORM_EPS) * norm_gain + norm_bias
    return normed.astype(jnp.bfloat16)


def any_groups(behaviors, candidates, ranks, lengths, hash_planes, norm_gain, norm_bias):
    group_rows = behaviors.shape[1]
    feature_width = behaviors.shape[2]
    own_cands = candidates.shape[1]
    code_bits = hash_planes.shape[1]
    seqs = lax.axis_size("seq")
    seq_index = lax.axis_index("seq")
    tail_rows = behaviors[:, group_rows - HALO :, :]
    before = lax.ppermute(tail_rows, "seq", [(k, (k + 1) % seqs) for k in range(seqs)])
    queries = lax.all_gather(candidates, "seq", axis=1, tiled=True)
    window_pos = ranks[:, 0, :]
    from_tail = window_pos < HALO
    tail_index = jnp.clip(window_pos, 0, HALO - 1)
    own_index = jnp.clip(window_pos - HALO, 0, group_rows - 1)
    take_rows = jax.vmap(lambda row_table, where_at: row_table[where_at])
    picked = jnp.where(
        from_tail[:, :, None], take_rows(before, tail_index), take_rows(behaviors, own_index)
    )
    position = seq_index * group_rows - HALO + window_pos
    usable = (position >= 0) & (position < lengths[:, None])
    query_codes, picked_codes = (
        jnp.tanh(
            jnp.einsum("ukd,db->ukb", rows, hash_planes, preferred_element_type=jnp.float32)
        ).astype(jnp.bfloat16)
        for rows in (queries, picked)
    )
    similar = jnp.einsum("ucd,ukd->uck", queries, picked, preferred_element_type=jnp.float32)
    agreement = jnp.einsum(
        "ucb,ukb->uck", query_codes, picked_codes, preferred_element_type=jnp.float32
    )
    scores = similar * (1.0 / math.sqrt(feature_width)) + HASH_WEIGHT / code_bits * agreement
    usable_rows = usable[:, None, :]
    group_max = jnp.max(jnp.where(usable_rows, scores, NEG_FILL), axis=2)
    weights = jnp.where(usable_rows, jnp.exp(scores - group_max[..., None]), 0.0)
    group_total = jnp.sum(weights, axis=2)
    group_sum = jnp.einsum(
        "uck,ukd->ucd", weights.astype(jnp.bfloat16), picked, preferred_element_type=jnp.float32
    )
    tops = lax.all_gather(group_max, "seq")
    rescales = jnp.exp(tops - jnp.max(tops, axis=0))
    numerator = jnp.sum(rescales[..., None] * lax.all_gather(group_sum, "seq"), axis=0)
    denominator = jnp.sum(rescales * lax.all_gather(group_total, "seq"), axis=0)
    attended = numerator / denominator[..., None]
    moments = user_total(
        jnp.stack([jnp.sum(attended, axis=(0, 1)), jnp.sum(attended * attended, axis=(0, 1))])
    )
    row_count = attended.shape[0] * attended.shape[1] * lax.axis_size("user")
    own = lax.dynamic_slice_in_dim(attended, seq_index * own_cands, own_cands, 1)
    return normalized(own, moments, row_count, norm_gain, norm_bias)


def load_kernel(
    ranks_hbm, lengths_hbm, norm_gain_hbm, norm_bias_hbm, planes_hbm, mine_hbm, behaviors_hbm,
    sent_ref, places_ref, gain_ref, bias_ref, planes_ref,
    ranks, lengths, sems,
):
    users, group_rows, _ = behaviors_hbm.shape
    tail = group_rows - HALO
    pairs = [
        *(
            (behaviors_hbm.at[user, pl.ds(tail, HALO)], sent_ref.at[user, pl.ds(0, HALO)])
            for user in range(users)
        ),
        (mine_hbm, sent_ref.at[:, pl.ds(HALO, mine_hbm.shape[1])]),
        (ranks_hbm, ranks),
        (lengths_hbm, lengths),
        (planes_hbm, planes_ref),
        (norm_gain_hbm, gain_ref),
        (norm_bias_hbm, bias_ref),
    ]
    copies = [
        pltpu.make_async_copy(source, target, sems.at[k])
        for k, (source, target) in enumerate(pairs)
    ]
    for copy in copies:
        copy.start()
    for copy in copies[users + 1 : users + 3]:
        copy.wait()
    start = lax.axis_index("seq") * group_rows - HALO
    for user in range(users):
        position = ranks[user] + start
        usable = (position >= 0) & (position < lengths[user])
        places_ref[user] = jnp.where(usable, ranks[user], HALO + group_rows)
    for copy in copies[: users + 1] + copies[users + 3 :]:
        copy.wait()


def own_picks_kernel(
    places_ref, rows_ref, sent_ref, planes_ref,
    picked_ref, picked_codes_ref, mine_codes_ref, masks_ref,
):
    users, group_rows, _ = rows_ref.shape
    picks = places_ref.shape[2]
    planes = planes_ref[...]
    lanes = lax.broadcasted_iota(jnp.int32, (picks, group_rows), 1)
    for user in range(users):
        places = places_ref[user]
        columns = jnp.transpose(jnp.broadcast_to(places, (picks, picks)))
        in_tail = (columns == lanes[:, :HALO]).astype(jnp.float32)
        masks_ref[user, 0:1] = ((places >= HALO) & (places < HALO + group_rows)).astype(jnp.float32)
        masks_ref[user, 1:2] = jnp.max(in_tail, axis=0, keepdims=True)
        wide = jnp.concatenate([columns - HALO] * (group_rows // picks), axis=1)
        chosen = (wide == lanes).astype(jnp.float32).astype(jnp.bfloat16)
        picked = jnp.dot(chosen, rows_ref[user], preferred_element_type=jnp.float32).astype(
            jnp.bfloat16
        )
        picked_ref[user] = picked
        picked_codes_ref[user] = soft_codes(picked, planes)
        mine_codes_ref[user] = soft_codes(sent_ref[user, HALO:], planes)


def attend_kernel(
    masks_ref, picked_ref, picked_codes_ref, sent_ref, mine_codes_ref, other_ref, planes_ref,
    part_ref,
):
    user_count, _, width = picked_ref.shape
    users = range(user_count)
    code_bits = planes_ref.shape[0]
    planes = planes_ref[...]
    codes = [soft_codes(other_ref[user], planes) for user in users]
    rows, similar = [], []
    for user in users:
        queries = jnp.concatenate([sent_ref[user, HALO:], other_ref[user, HALO:]], axis=0)
        rows.append(jnp.concatenate([picked_ref[user], other_ref[user, :HALO]], axis=0))
        similar.append(last_with_last(queries, rows[user]) * (1.0 / math.sqrt(width)))
    scores, usable = [], []
    for user in users:
        query_codes = jnp.concatenate([mine_codes_ref[user], codes[user][HALO:]], axis=0)
        row_codes = jnp.concatenate([picked_codes_ref[user], codes[user][:HALO]], axis=0)
        agreement = last_with_last(query_codes, row_codes)
        scores.append(similar[user] + HASH_WEIGHT / code_bits * agreement)
        usable.append(
            jnp.concatenate([masks_ref[user, 0:1], masks_ref[user, 1:2]], axis=1) > 0.0
        )
    group_max = [
        jnp.max(jnp.where(usable[user], scores[user], NEG_FILL), axis=1, keepdims=True)
        for user in users
    ]
    weights = [
        jnp.where(usable[user], jnp.exp(scores[user] - group_max[user]), 0.0) for user in users
    ]
    for user in users:
        part_ref[user, :, :width] = jnp.dot(
            weights[user].astype(jnp.bfloat16), rows[user], preferred_element_type=jnp.float32
        )
    for user in users:
        group_total = jnp.sum(weights[user], axis=1, keepdims=True)
        side_lane = lax.broadcasted_iota(jnp.int32, (group_total.shape[0], SIDE), 1)
        part_ref[user, :, width:] = jnp.where(
            side_lane < SIDE // 2, group_max[user], group_total
        )


def merge_kernel(mine_ref, other_ref, own_ref, moments_ref):
    users, cands, packed = mine_ref.shape
    width = packed - SIDE
    half = cands // 2
    low = lax.broadcasted_iota(jnp.int32, (half, SIDE), 1) < SIDE // 2
    sums, squares = [], []
    for user in range(users):
        for first in (0, half):
            here = (user, slice(first, first + half))
            there = (user, slice(half - first, cands - first))
            tops, totals = [], []
            for ref, at in ((mine_ref, here), (other_ref, there)):
                side = ref[at[0], at[1], width:]
                turned = pltpu.roll(side, SIDE // 2, 1)
                tops.append(jnp.where(low, side, turned))
                totals.append(jnp.where(low, turned, side))
            joint_max = jnp.maximum(*tops)
            scales = [jnp.exp(top - joint_max) for top in tops]
            denominator = scales[0] * totals[0] + scales[1] * totals[1]
            for column in range(0, width, SIDE):
                lanes = slice(column, column + SIDE)
                numerator = (
                    scales[0] * mine_ref[here[0], here[1], lanes]
                    + scales[1] * other_ref[there[0], there[1], lanes]
                )
                attended = numerator / denominator
                sums.append((column, jnp.sum(attended, axis=0, keepdims=True)))
                squares.append((column, jnp.sum(attended * attended, axis=0, keepdims=True)))
                if first == 0:
                    own_ref[user, :, lanes] = attended
    for row, terms in enumerate((sums, squares)):
        for column in range(0, width, SIDE):
            moments_ref[row : row + 1, column : column + SIDE] = sum(
                term for at, term in terms if at == column
            )


def two_groups(behaviors, candidates, ranks, lengths, hash_planes, norm_gain, norm_bias):
    users, group_rows, width = behaviors.shape
    own_cands = candidates.shape[1]
    picks = ranks.shape[2]
    cands = 2 * own_cands
    f32, bf16 = jnp.float32, jnp.bfloat16
    in_vmem = pl.BlockSpec(memory_space=pltpu.VMEM)
    swap = [(0, 1), (1, 0)]
    bits = hash_planes.shape[1]
    arguments = (ranks, lengths, norm_gain, norm_bias, hash_planes.T, candidates, behaviors)
    params = pltpu.CompilerParams(vmem_limit_bytes=VMEM_LIMIT)
    scheduled = pltpu.CompilerParams(
        vmem_limit_bytes=VMEM_LIMIT
    )
    sent_bytes = 2 * users * (HALO + own_cands) * width
    sent, places, gain, bias, planes = pl.pallas_call(
        load_kernel,
        out_shape=(
            jax.ShapeDtypeStruct((users, HALO + own_cands, width), bf16),
            jax.ShapeDtypeStruct(ranks.shape, jnp.int32),
            jax.ShapeDtypeStruct(norm_gain.shape, f32),
            jax.ShapeDtypeStruct(norm_bias.shape, f32),
            jax.ShapeDtypeStruct((bits, width), bf16),
        ),
        in_specs=[pl.BlockSpec(memory_space=pl.ANY)] * len(arguments),
        out_specs=(in_vmem,) * 5,
        scratch_shapes=[
            pltpu.VMEM(ranks.shape, jnp.int32),
            pltpu.SMEM(lengths.shape, jnp.int32),
            pltpu.SemaphoreType.DMA((len(arguments) + users - 1,)),
        ],
        cost_estimate=pl.CostEstimate(flops=LOAD_COST, bytes_accessed=sent_bytes, transcendentals=0),
        compiler_params=params,
        name="load",
    )(*(pltpu.with_memory_space_constraint(value, pltpu.HBM) for value in arguments))
    other = lax.ppermute(sent, "seq", swap)
    picked, picked_codes, mine_codes, masks = pl.pallas_call(
        own_picks_kernel,
        out_shape=(
            jax.ShapeDtypeStruct((users, picks, width), bf16),
            jax.ShapeDtypeStruct((users, picks, bits), bf16),
            jax.ShapeDtypeStruct((users, own_cands, bits), bf16),
            jax.ShapeDtypeStruct((users, 2, picks), f32),
        ),
        in_specs=[in_vmem] * 4,
        out_specs=(in_vmem,) * 4,
        cost_estimate=pl.CostEstimate(
            flops=2 * users * picks * group_rows * width,
            bytes_accessed=behaviors.nbytes,
            transcendentals=0,
        ),
        compiler_params=scheduled,
        name="own_picks",
    )(places, behaviors, sent, planes)
    part = pl.pallas_call(
        attend_kernel,
        out_shape=jax.ShapeDtypeStruct((users, cands, width + SIDE), f32),
        in_specs=[in_vmem] * 7,
        out_specs=in_vmem,
        compiler_params=scheduled,
        name="attend",
    )(masks, picked, picked_codes, sent, mine_codes, other, planes)
    own, moments = pl.pallas_call(
        merge_kernel,
        out_shape=(
            jax.ShapeDtypeStruct((users, own_cands, width), f32),
            jax.ShapeDtypeStruct((2, width), f32),
        ),
        in_specs=[in_vmem] * 2,
        out_specs=(in_vmem,) * 2,
        compiler_params=scheduled,
        name="merge",
    )(part, lax.ppermute(part, "seq", swap))
    row_count = users * cands * lax.axis_size("user")
    return normalized(own, user_total(moments), row_count, gain, bias)


def solution(mesh):
    in_specs = (
        P("user", "seq", None),
        P("user", "seq", None),
        P("user", "seq", None),
        P("user"),
        P(),
        P(),
        P(),
    )
    out_specs = P("user", "seq", None)
    shards = two_groups if mesh.shape["seq"] == 2 else any_groups
    return jax.shard_map(shards, mesh=mesh, in_specs=in_specs, out_specs=out_specs, check_vma=False)
```
